32 devices in a mesh: dev: 8 (over z, x), rep: 4 (over y, core).
Axes of the slice: x: 2, y: 2, z: 4, core: 2. Of those that a mesh axis runs over, the one named last changes fastest.
Arguments:
- h_zero: bfloat16 [32768, 256], P(('dev', 'rep')), may hold values from 0 to 2
- h_prev: bfloat16 [32768, 256], P(('dev', 'rep')), may hold values from 0 to 2
- hist_a: bfloat16 [32768, 256], P('dev'), may hold values from 0 to 2
- hist_b: bfloat16 [32768, 256], P('dev'), may hold values from 0 to 2
- tile_vals: bfloat16 [256, 12, 128, 128], P(('dev', 'rep'))
- tile_cols: int32 [256, 12], P(('dev', 'rep')), may hold values from 0 to 47, as said below
- pull_rows: int32 [32, 8, 128], P(('dev', 'rep')), may hold values from 0 to 4095
- pull_counts: int32 [32, 8], P(('dev', 'rep')), may hold values from 96 to 128, as said below
- weight_two: bfloat16 [256, 256], replicated, may hold values from -0.375 to 0.375
- weight_three: bfloat16 [256, 256], replicated, may hold values from -0.375 to 0.375
- grad_out: bfloat16 [32768, 256], P(('dev', 'rep')), may hold values from -0.125 to 0.125
Outputs:
- layer_three: bfloat16 [32768, 256], P(('dev', 'rep'))
- new_history: bfloat16 [32768, 256], P('dev')
- weight_grad: float32 [256, 256], replicated
The draws below stay inside these ranges and needn't reach their ends.
Inputs may be any that keep to these rules, and one draw needn't show every extreme that they name: `tile_cols`: entry 0 of a row block names one of its device's own 8 blocks; entries 1 to 3 name blocks of the owner's history shard; the other 8 name pulled blocks of consecutive owners modulo 8, and every owner's block is named by some row block of each device. `pull_rows`: entries at slots at or past the block's count are read by no output. `pull_counts`: every device pulls a full block of 128 rows from some owner and a block of exactly 96 rows from another.
All inputs are finite; a program needn't handle non-finite values.
Results may differ from the reference program's by a relative error of at most 0.0034.
Values may be sent and summed in bfloat16 or wider, within the bound.
A program may use at most 128 MiB of HBM per device.

```python
import math
import jax
import jax.numpy as jnp
from jax import lax

WIDTH = 256
BATCH = 1024
TILE = 128
HOME_TILES = 3
REMOTE_TILES = 8
TPR = 12
ROWBLK = 8
WORKERS = 32
SHARD = 4096
NODES = 32768
N_DEV = 8
N_REP = 4


def draw_tile_vals(key, part):
    full_shape = (WORKERS * ROWBLK, TPR, TILE, TILE)
    key_mask, key_value = jax.random.split(key, 2)
    edge_mask = jax.random.bernoulli(key_mask, 0.125, full_shape).astype(jnp.float32)
    edge_weight = jax.random.uniform(key_value, full_shape, jnp.float32, 0.5, 1.5)
    return (edge_mask * edge_weight * (8.0 / (TPR * TILE))).astype(jnp.bfloat16)


def draw_tile_cols(key, part):
    key_local, key_home, key_shift = jax.random.split(key, 3)
    row_count = WORKERS * ROWBLK
    local_cols = jax.random.randint(key_local, (row_count, 1), 0, ROWBLK, jnp.int32)
    home_cols = jax.random.randint(key_home, (row_count, HOME_TILES), ROWBLK, ROWBLK + N_REP * ROWBLK, jnp.int32)
    shifts = jax.random.randint(key_shift, (WORKERS, 1), 0, N_DEV, jnp.int32)
    shift_rows = jnp.repeat(shifts, ROWBLK, axis=0)
    block_pos = (jnp.arange(row_count, dtype=jnp.int32) % ROWBLK)[:, None]
    slot_pos = jnp.arange(REMOTE_TILES, dtype=jnp.int32)[None, :]
    peer_ids = (block_pos * REMOTE_TILES + slot_pos + shift_rows) % N_DEV
    remote_cols = ROWBLK + N_REP * ROWBLK + peer_ids
    return jnp.concatenate([local_cols, home_cols, remote_cols], axis=1).astype(jnp.int32)


def draw_pull_counts(key, part):
    key_one, key_two, key_full = jax.random.split(key, 3)
    full_shape = (WORKERS, N_DEV)
    first = jax.random.randint(key_one, full_shape, 1, TILE + 1, jnp.int32)
    second = jax.random.randint(key_two, full_shape, 1, TILE + 1, jnp.int32)
    counts = TILE - first * second // (4 * TILE)
    offset = jax.random.randint(key_full, (), 0, N_DEV, jnp.int32)
    full_peer = (jnp.arange(WORKERS, dtype=jnp.int32) * 5 + offset) % N_DEV
    low_peer = (full_peer + 1) % N_DEV
    peer_ids = jnp.arange(N_DEV, dtype=jnp.int32)[None, :]
    counts = jnp.where(peer_ids == low_peer[:, None], TILE - TILE // 4, counts)
    counts = jnp.where(peer_ids == full_peer[:, None], TILE, counts)
    return counts.astype(jnp.int32)


def set_ends(drawn, stream_key, low, top_value):
    spot = [jax.random.randint(jax.random.fold_in(stream_key, axis), (), 0, length) for axis, length in enumerate(drawn.shape)]
    longest = drawn.shape.index(max(drawn.shape))
    next_to = spot[:longest] + [(spot[longest] + 1) % drawn.shape[longest]] + spot[longest + 1:]
    return drawn.at[tuple(spot)].set(low).at[tuple(next_to)].set(top_value)


def levels(rng, dims, cuts, low, top_value):
    gain = 1.0
    for axis_at, parts in cuts:
        draws = jax.random.uniform(jax.random.fold_in(jax.random.fold_in(rng, 6), axis_at), (parts,), jnp.float32, low / len(cuts), top_value / len(cuts))
        gain = gain * jnp.repeat(jnp.exp(draws), dims[axis_at] // parts).reshape((-1,) + (1,) * (len(dims) - 1 - axis_at))
    return gain


def gaussian(key, extent, spread, most, pieces=(), kind=jnp.bfloat16):
    level = levels(key, extent, pieces, -0.22, 0.18) if pieces else 1.0
    entries = jax.random.normal(key, extent, jnp.float32) * spread * level
    return jnp.minimum(jnp.maximum(entries, -most), most).astype(kind)


def setup_inputs(seed: int = 0) -> dict:
    key_list = jax.random.split(jax.random.key(seed), 12)
    return {
        "h_zero": jnp.clip(2.0 * jax.random.uniform(key_list[0], (NODES, WIDTH), jnp.float32) ** levels(key_list[0], (NODES, WIDTH), ((0, 32),), -0.2, 0.2), 0.0, 2.0).astype(jnp.bfloat16),
        "h_prev": jnp.clip(2.0 * jax.random.uniform(key_list[1], (NODES, WIDTH), jnp.float32) ** levels(key_list[1], (NODES, WIDTH), ((0, 32),), -0.2, 0.2), 0.0, 2.0).astype(jnp.bfloat16),
        "hist_a": jnp.clip(2.0 * jax.random.uniform(key_list[2], (NODES, WIDTH), jnp.float32) ** levels(key_list[2], (NODES, WIDTH), ((0, 8),), -0.2, 0.2), 0.0, 2.0).astype(jnp.bfloat16),
        "hist_b": jnp.clip(2.0 * jax.random.uniform(key_list[3], (NODES, WIDTH), jnp.float32) ** levels(key_list[3], (NODES, WIDTH), ((0, 8),), -0.2, 0.2), 0.0, 2.0).astype(jnp.bfloat16),
        "tile_vals": draw_tile_vals(jax.random.fold_in(key_list[11], 71), 0),
        "tile_cols": draw_tile_cols(jax.random.fold_in(key_list[11], 71), 0),
        "pull_rows": set_ends(jax.random.randint(key_list[6], (WORKERS, N_DEV, TILE), 0, SHARD), jax.random.fold_in(key_list[6], 1), 0, SHARD - 1).astype(jnp.int32),
        "pull_counts": draw_pull_counts(jax.random.fold_in(key_list[11], 71), 0),
        "weight_two": gaussian(key_list[8], (WIDTH, WIDTH), WIDTH ** -0.5, 0.375),
        "weight_three": gaussian(key_list[9], (WIDTH, WIDTH), WIDTH ** -0.5, 0.375),
        "grad_out": gaussian(key_list[10], (NODES, WIDTH), (4.0 / NODES ** 0.5), 0.125, ((0, 32),)),
    }


restart = 0.1
strength = 0.5


def propagate(current, history, pulled, values, columns, start_rows, weight, layer_number):
    feature_width = current.shape[1]
    source = jnp.concatenate([current, history, pulled.reshape(-1, feature_width)], axis=0)
    blocks = source.reshape(-1, TILE, feature_width)
    picked = jnp.take(blocks, columns.reshape(-1), axis=0).reshape(columns.shape + (TILE, feature_width))
    summed = jnp.einsum("btij,btjf->bif", values.astype(jnp.float32), picked.astype(jnp.float32))
    summed = summed.reshape(current.shape[0], feature_width)
    mixed_rows = (1.0 - restart) * summed + restart * start_rows.astype(jnp.float32)
    mixed_low = mixed_rows.astype(jnp.bfloat16)
    factor = math.log(strength / layer_number + 1.0)
    product = jnp.dot(mixed_low, weight, preferred_element_type=jnp.float32)
    inner_sum = (1.0 - factor) * mixed_rows + factor * product
    return jnp.maximum(inner_sum, 0.0).astype(jnp.bfloat16), mixed_low


def reference(h_zero, h_prev, hist_a, hist_b, tile_vals, tile_cols, pull_rows, pull_counts, weight_two, weight_three, grad_out):
    shard_a = hist_a.reshape(N_DEV, SHARD, WIDTH)
    shard_b = hist_b.reshape(N_DEV, SHARD, WIDTH)
    owners = jnp.arange(N_DEV, dtype=jnp.int32)[:, None]
    slot_ids = jnp.arange(TILE, dtype=jnp.int32)[None, :]

    def device(items):
        worker, start_rows, current, values, columns, wanted, counts, upstream = items
        home_shard = (worker // N_REP).astype(jnp.int32)
        live_mask = (slot_ids < counts[:, None])[:, :, None]
        pulled_a = jnp.where(live_mask, shard_a[owners, wanted], jnp.zeros((), shard_a.dtype))
        pulled_b = jnp.where(live_mask, shard_b[owners, wanted], jnp.zeros((), shard_b.dtype))
        own_a = lax.dynamic_index_in_dim(shard_a, home_shard, 0, keepdims=False)
        own_b = lax.dynamic_index_in_dim(shard_b, home_shard, 0, keepdims=False)
        second, unused_mix = propagate(current, own_a, pulled_a, values, columns, start_rows, weight_two, 2)
        layer_out, mixed_low = propagate(second, own_b, pulled_b, values, columns, start_rows, weight_three, 3)
        factor = math.log(strength / 3 + 1.0)
        grad_term = factor * jnp.dot(mixed_low.T, upstream, preferred_element_type=jnp.float32)
        return layer_out, second, grad_term

    items = (
        jnp.arange(WORKERS, dtype=jnp.int32),
        h_zero.reshape(WORKERS, BATCH, WIDTH),
        h_prev.reshape(WORKERS, BATCH, WIDTH),
        tile_vals.reshape(WORKERS, ROWBLK, TPR, TILE, TILE),
        tile_cols.reshape(WORKERS, ROWBLK, TPR),
        pull_rows,
        pull_counts,
        grad_out.reshape(WORKERS, BATCH, WIDTH),
    )
    layer_out, second, grad_terms = lax.map(device, items)
    return layer_out.reshape(NODES, WIDTH), second.reshape(NODES, WIDTH), jnp.sum(grad_terms, axis=0)
```

```python
import functools
import math

import jax
import jax.numpy as jnp
from jax import lax
from jax.experimental import pallas as pl
from jax.experimental.pallas import tpu as pltpu
from jax.sharding import PartitionSpec as P

restart = 0.1
strength = 0.5
MESH = pl.DeviceIdType.MESH
scope = jax.named_scope


def kernel(
    D, R,
    cols_h, counts_h, rows_h,
    h_zero, h_prev, hist_a, hist_b, tile_vals, w_two, w_three, grad_out,
    layer_out, hist_out, grad_res,
    cols, counts, rows_in,
    zero_v, cur_v, hist_av, hist_bv, vals_v, far_v, w2_v, w3_v, up_v,
    ask, asked, col, send_a, send_b, pull_a, pull_b, acc, acc_a, acc_b,
    fresh_v, low_v, g_send, g_mate, g_recv, g_part, g_all,
    local_sem, stage_sem, idx_s, idx_r, a_s, a_r, b_s, b_r, f_s, f_r, m_s, m_r, g_s, g_r, p_s, p_r,
):
    N = D * R
    X = 2 if D % 2 == 0 else 1
    Z = D // X
    H = Z // 2
    d = lax.axis_index("dev")
    r = lax.axis_index("rep")
    z, x = lax.div(d, X), lax.rem(d, X)
    me = d * R + r
    slots = rows_in.shape[2]
    feat = hist_av.shape[2]
    blocks = vals_v.shape[0]
    tiles = vals_v.shape[1]
    home = 4
    home_blocks = hist_av.shape[0]
    far_base = blocks + home_blocks
    dense = tiles - home == D

    barrier = pltpu.get_barrier_semaphore()
    if R == 4:
        side = lax.rem(r, 2)
        mates = [r + 1 - 2 * side, lax.rem(r + 2, R)]
    else:
        side = lax.rem(r, 2)
        mates = [lax.rem(r + 1 + k, R) for k in range(R - 1)]

    def signal_dev(sem):
        for step in (1, -1):
            t = z + step

            @pl.when(jnp.logical_and(t >= 0, t < Z))
            def _():
                pl.semaphore_signal(sem, inc=1, device_id=(t * X + x, r), device_id_type=MESH)

        if X == 2:
            pl.semaphore_signal(sem, inc=1, device_id=(z * X + 1 - x, r), device_id_type=MESH)

    def wait_dev(sem, more):
        inner = lax.div(z + Z - 1, Z) + lax.div(2 * Z - 2 - z, Z)
        pl.semaphore_wait(sem, inner + X - 1 + more)

    def signal_rep(sem):
        for t in mates:
            pl.semaphore_signal(sem, inc=1, device_id=(d, t), device_id_type=MESH)

    signal_dev(barrier)
    signal_rep(barrier)

    loads = [
        (rows_h, rows_in), (counts_h, counts), (hist_a, hist_av), (tile_vals, vals_v), (cols_h, cols),
        (hist_b, hist_bv), (h_prev, cur_v), (h_zero, zero_v), (w_two, w2_v), (w_three, w3_v), (grad_out, up_v),
    ]
    copies = [pltpu.make_async_copy(s, t, local_sem.at[i]) for i, (s, t) in enumerate(loads)]
    for c in copies:
        c.start()
    copies[0].wait()
    copies[1].wait()

    lane = lax.broadcasted_iota(jnp.int32, (1, slots), 1)

    def mask_rows(p, _):
        ask[p] = jnp.where(lane < counts[0, p], rows_in[0, pl.ds(p, 1), :], -1)
        return 0

    lax.fori_loop(0, D, mask_rows, 0)

    def ask_peer(p):
        pltpu.make_async_remote_copy(
            src_ref=ask.at[p], dst_ref=asked.at[d], send_sem=idx_s.at[p], recv_sem=idx_r.at[d],
            device_id=(p, r), device_id_type=MESH,
        ).start()

    def ask_at(s):
        for step in (1, -1):
            t = z + step * (s + 1)

            @pl.when(jnp.logical_and(t >= 0, t < Z))
            def _():
                ask_peer(t * X + x)

            if X == 2:
                u = z + step * s
                ok = jnp.logical_and(u >= 0, u < Z)
                ok = jnp.logical_and(ok, s + (1 + step) > 0)

                @pl.when(ok)
                def _():
                    ask_peer(u * X + 1 - x)

    rounds = Z - 1 + X - 1
    with scope("stages"):
        wait_dev(barrier, len(mates))
        signal_dev(stage_sem.at[0])
        ask_at(0)

        def stage(s, _):
            wait_dev(stage_sem.at[s - 1], 0)

            @pl.when(s < rounds - 1)
            def _():
                signal_dev(stage_sem.at[s])

            ask_at(s)
            return 0

        for s in range(1, rounds) if rounds < 6 else ():
            stage(s, 0)
        if rounds >= 6:
            lax.fori_loop(1, rounds, stage, 0)
    signal_rep(stage_sem.at[rounds])
    asked[d] = ask[d]

    def plane(m):
        if Z % 2:
            return lax.rem(z + 1 + m, Z)
        up = lax.div(z, H)
        over = (1 - up) * (H + m) + up * (H - 1 - m)
        near = up * H + lax.rem(z - up * H + 1 + m, H)
        far = lax.div(m, H)
        return (1 - far) * over + far * near

    if dense:
        copies[3].wait()
        copies[4].wait()

        def spread_tiles(i, _):
            first = cols[i, home] - far_base
            for p in range(D):
                t = home + lax.rem(p - first + D, D)
                far_v[p // X, pl.ds(i * slots, slots), (p % X) * slots:(p % X + 1) * slots] = vals_v[i, t]
            return 0

        with scope("tiles"):
            lax.fori_loop(0, blocks, spread_tiles, 0)

    group = X
    chunk_blocks = 8
    depth = chunk_blocks * slots
    lanes = lax.broadcasted_iota(jnp.int32, (group * slots, depth), 1)

    def idx_copy(q):
        return pltpu.make_async_remote_copy(
            src_ref=ask.at[q], dst_ref=asked.at[q], send_sem=idx_s.at[q], recv_sem=idx_r.at[q],
            device_id=(q, r), device_id_type=MESH,
        )

    def gather(table, send_buf, pull_buf, s, q_sem, fresh_keys):
        def one_group(m, _):
            base = plane(m) * X
            if fresh_keys:
                for e in range(X):
                    q = base + e

                    @pl.when(q != d)
                    def _():
                        idx_copy(q).wait_recv()

                    col[q] = jnp.broadcast_to(asked[q], (slots, slots)).T
            keys = col[pl.ds(base, group)].reshape(group * slots, slots)
            wide = jnp.concatenate([keys] * chunk_blocks, axis=1)

            def one_chunk(k, _):
                hot = jnp.where(wide - k * depth == lanes, 1.0, 0.0).astype(jnp.bfloat16)
                part = table[pl.ds(k * chunk_blocks, chunk_blocks)].reshape(depth, feat)
                found = jnp.dot(hot, part, preferred_element_type=jnp.float32)

                @pl.when(k == 0)
                def _():
                    acc[...] = found

                @pl.when(k > 0)
                def _():
                    acc[...] += found

                return 0

            lax.fori_loop(0, home_blocks // chunk_blocks, one_chunk, 0)
            send_buf[pl.ds(base, group)] = (
                acc[...].astype(jnp.bfloat16).reshape(group, slots, feat)
            )
            for e in range(X):
                q = base + e

                @pl.when(q != d)
                def _():
                    pltpu.make_async_remote_copy(
                        src_ref=send_buf.at[q], dst_ref=pull_buf.at[d], send_sem=s.at[q],
                        recv_sem=q_sem.at[d], device_id=(q, r), device_id_type=MESH,
                    ).start()

            return 0

        lax.fori_loop(0, Z, one_group, 0)
        pull_buf[d] = send_buf[d]

    def block_copy(send_buf, pull_buf, s, q_sem, p):
        return pltpu.make_async_remote_copy(
            src_ref=send_buf.at[p], dst_ref=pull_buf.at[p], send_sem=s.at[p], recv_sem=q_sem.at[p],
            device_id=(p, r), device_id_type=MESH,
        )

    copies[2].wait()
    with scope("gather_a"):
        gather(hist_av, send_a, pull_a, a_s, a_r, True)
    copies[5].wait()
    with scope("gather_b"):
        gather(hist_bv, send_b, pull_b, b_s, b_r, False)
    waited = (0, 1, 2, 3, 4, 5) if dense else (0, 1, 2, 5)
    for i in range(len(copies)):
        if i not in waited:
            copies[i].wait()

    def product(i, picks):
        left = jnp.concatenate([vals_v[i, t] for t, _ in picks], axis=1)
        right = jnp.concatenate([b for _, b in picks], axis=0)
        return jnp.dot(left, right, preferred_element_type=jnp.float32)

    def near_tiles(i, _):
        picks = [(0, cur_v[cols[i, 0]])]
        picks += [(t, hist_av[jnp.maximum(cols[i, t] - blocks, 0)]) for t in range(1, home)]
        acc_a[i] = product(i, picks)
        acc_b[i] = product(i, [(t, hist_bv[jnp.maximum(cols[i, t] - blocks, 0)]) for t in range(1, home)])
        return 0

    with scope("near"):
        lax.fori_loop(0, blocks, near_tiles, 0)

    pl.semaphore_wait(stage_sem.at[rounds], len(mates))
    if R == 4:
        signal_rep(stage_sem.at[rounds + 1])
        pl.semaphore_wait(stage_sem.at[rounds + 1], len(mates))

    rows = blocks * slots

    def pull_plane(n, acc_ref, send_buf, pull_buf, s, q_sem):
        m = lax.rem(n + Z - 1, Z) if Z % 2 else lax.rem(n + H + (Z - 1 - H), Z)
        if Z % 2 == 0:
            m = jnp.where(n == 0, Z - 1, jnp.where(n < H, H + n - 1, n - H))
        zt = plane(m)
        for e in range(X):
            q = zt * X + e

            @pl.when(q != d)
            def _():
                block_copy(send_buf, pull_buf, s, q_sem, q).wait_recv()

        part = jnp.dot(
            far_v[zt], pull_buf[pl.ds(zt * X, X)].reshape(X * slots, feat),
            preferred_element_type=jnp.float32,
        )
        acc_ref[...] += part.reshape(blocks, slots, feat)

    def pull_all(acc_ref, send_buf, pull_buf, s, q_sem):
        if dense:
            for n in range(Z):
                pull_plane(n, acc_ref, send_buf, pull_buf, s, q_sem)
            return

        def one(k, _):
            p = lax.rem(d + 1 + k, D)
            block_copy(send_buf, pull_buf, s, q_sem, p).wait_recv()
            return 0

        lax.fori_loop(0, D - 1, one, 0)

        def far(i, _):
            acc_ref[i] += product(
                i, [(t, pull_buf[jnp.maximum(cols[i, t] - far_base, 0)]) for t in range(home, tiles)]
            )
            return 0

        lax.fori_loop(0, blocks, far, 0)

    factor_two = math.log(strength / 2 + 1.0)
    factor_three = math.log(strength / 3 + 1.0)

    def mix(acc_ref, at):
        return (1.0 - restart) * acc_ref[at] + restart * zero_v[at].astype(jnp.float32)

    def activate(mixed, low, w, factor):
        shape = mixed.shape
        prod = jnp.dot(low.reshape(-1, feat), w[...], preferred_element_type=jnp.float32)
        inner = (1.0 - factor) * mixed + factor * prod.reshape(shape)
        return jnp.maximum(inner, 0.0).astype(jnp.bfloat16)

    with scope("pull_a"):
        pull_all(acc_a, send_a, pull_a, a_s, a_r)

    step = 2 if blocks % 2 == 0 else 1
    pieces = blocks // step

    def fresh_copy(slot, target, k, c):
        at = pl.ds(c * step, step)
        return pltpu.make_async_remote_copy(
            src_ref=hist_out.at[slot, at], dst_ref=hist_out.at[slot, at], send_sem=f_s.at[k, c],
            recv_sem=f_r.at[k, c], device_id=(d, target), device_id_type=MESH,
        )

    if R == 4:
        mate, across = mates
        targets = [across, mate]
    else:
        mate, across = r + 1 - 2 * side, None
        targets = mates

    def second(c, _):
        at = pl.ds(c * step, step)
        mixed = mix(acc_a, at)
        made = activate(mixed, mixed.astype(jnp.bfloat16), w2_v, factor_two)
        fresh_v[at] = made
        hist_out[r, at] = made
        return 0

    with scope("second"):
        lax.fori_loop(0, pieces, second, 0)

        def send_fresh(c, _):
            for k, t in enumerate(targets):
                fresh_copy(r, t, k, c).start()
            return 0

        lax.fori_loop(0, pieces, send_fresh, 0)

    def own_tile(i, _):
        acc_b[i] += product(i, [(0, fresh_v[cols[i, 0]])])
        return 0

    with scope("own"):
        lax.fori_loop(0, blocks, own_tile, 0)

    with scope("pull_b"):
        pull_all(acc_b, send_b, pull_b, b_s, b_r)

    with scope("grad"):
        low_v[...] = mix(acc_b, slice(None)).astype(jnp.bfloat16)
        grad = factor_three * lax.dot_general(
            low_v[...].reshape(rows, feat), up_v[...].reshape(rows, feat),
            (((0,), (0,)), ((), ())), preferred_element_type=jnp.float32,
        )
        half = N // 2
        piece = g_send.shape[2]
        for c in range(N):
            g_send[c // half, c % half] = grad[c * piece:(c + 1) * piece, :]
    place = d * (R // 2) + lax.div(r, 2)
    to_mate = pltpu.make_async_remote_copy(
        src_ref=g_send.at[1 - side], dst_ref=g_mate, send_sem=m_s, recv_sem=m_r,
        device_id=(d, mate), device_id_type=MESH,
    )
    to_mate.start()

    def third(c, _):
        at = pl.ds(c * step, step)
        layer_out[at] = activate(mix(acc_b, at), low_v[at], w3_v, factor_three)
        return 0

    with scope("third"):
        lax.fori_loop(0, pieces, third, 0)

    def whole(ref, n, s, q):
        part = ref.at[pl.ds(0, n)]
        return pltpu.make_async_remote_copy(
            src_ref=part, dst_ref=part, send_sem=s, recv_sem=q,
            device_id=(lax.rem(d + 1, D), r), device_id_type=MESH,
        )

    with scope("mate"):
        to_mate.wait_recv()
    g_mate[...] += g_send[side]

    def scatter(k, _):
        t = lax.rem(place + 1 + k, half)
        pltpu.make_async_remote_copy(
            src_ref=g_mate.at[t], dst_ref=g_recv.at[place], send_sem=g_s, recv_sem=g_r,
            device_id=(lax.div(t, R // 2), 2 * lax.rem(t, R // 2) + side), device_id_type=MESH,
        ).start()
        return 0

    lax.fori_loop(0, half - 1, scatter, 0)
    g_recv[place] = g_mate[place]
    with scope("scatter"):
        whole(g_recv, half - 1, g_s, g_r).wait_recv()

    g_part[...] = jnp.sum(g_recv[...], axis=0).astype(g_part.dtype)
    mine = side * half + place

    def spread(k, _):
        t = lax.rem(me + 1 + k, N)
        pltpu.make_async_remote_copy(
            src_ref=g_part, dst_ref=g_all.at[mine], send_sem=p_s, recv_sem=p_r,
            device_id=(lax.div(t, R), lax.rem(t, R)), device_id_type=MESH,
        ).start()
        return 0

    lax.fori_loop(0, N - 1, spread, 0)
    g_all[mine] = g_part[...]

    if R == 4:
        def forward(c, _):
            fresh_copy(across, across, 0, c).wait_recv()
            fresh_copy(across, mate, 2, c).start()
            return 0

        with scope("forward"):
            lax.fori_loop(0, pieces, forward, 0)
    with scope("spread"):
        whole(g_all, N - 1, p_s, p_r).wait_recv()
    grad_res[...] = g_all[...].astype(jnp.float32)

    def drain(c, _):
        if R == 4:
            fresh_copy(r, mate, 1, c).wait_recv()
            fresh_copy(r, mate, 2, c).wait_recv()
            for k in range(3):
                fresh_copy(r, mate, k, c).wait_send()
        else:
            for k in range(R - 1):
                fresh_copy(r, mate, k, c).wait()
        return 0

    with scope("drain"):
        lax.fori_loop(0, pieces, drain, 0)

        def sent(k, _):
            p = lax.rem(d + 1 + k, D)
            idx_copy(p).wait_send()
            block_copy(send_a, pull_a, a_s, a_r, p).wait_send()
            block_copy(send_b, pull_b, b_s, b_r, p).wait_send()
            return 0

        lax.fori_loop(0, D - 1, sent, 0)
        to_mate.wait_send()
        whole(g_recv, half - 1, g_s, g_r).wait_send()
        whole(g_all, N - 1, p_s, p_r).wait_send()


def hand_over(parts, *refs):
    sources, targets, sem = refs[:3], refs[3:6], refs[6]
    outs = []
    for n, src, dst in zip(parts, sources, targets):
        rows = src.shape[0] // n
        for i in range(n):
            at = pl.ds(i * rows, rows)
            outs.append(pltpu.make_async_copy(src.at[at], dst.at[at], sem.at[len(outs)]))
    for c in outs:
        c.start()
    for c in outs:
        c.wait()


def local(D, R, h_zero, h_prev, hist_a, hist_b, tile_vals, tile_cols, pull_rows, pull_counts,
          weight_two, weight_three, grad_out):
    blocks, tiles, tile = tile_vals.shape[:3]
    feat = hist_a.shape[1]
    N = D * R
    hist_blocks = hist_a.shape[0] // tile
    piece = feat // N
    bf, f32 = jnp.bfloat16, jnp.float32
    own = (blocks, tile, feat)
    hist = (hist_blocks, tile, feat)
    slots = pull_rows.shape[2]
    pulled = (D, slots, feat)
    X = 2 if D % 2 == 0 else 1
    Z = D // X
    dense = tiles - 4 == D
    far = (Z, blocks * tile, X * tile) if dense else (1, 16, 128)
    pieces = blocks // 2 if blocks % 2 == 0 else blocks
    links = max(R - 1, 3)
    vm = pltpu.VMEM
    dma = pltpu.SemaphoreType.DMA
    any_spec = pl.BlockSpec(memory_space=pl.ANY)
    vspec = pl.BlockSpec(memory_space=pltpu.VMEM)
    grant = 24 * 2**20 + D * slots * (8 * feat + 4 * slots)
    out3, fresh, grad = pl.pallas_call(
        functools.partial(kernel, D, R),
        out_shape=(
            jax.ShapeDtypeStruct(own, bf),
            jax.ShapeDtypeStruct((R,) + own, bf),
            jax.ShapeDtypeStruct((N, piece, feat), f32),
        ),
        in_specs=[any_spec] * 11,
        out_specs=(vspec, vspec, vspec),
        scratch_shapes=[
            pltpu.SMEM(tile_cols.shape, jnp.int32), pltpu.SMEM(pull_counts.shape, jnp.int32),
            vm(pull_rows.shape, jnp.int32),
            vm(own, bf), vm(own, bf), vm(hist, bf), vm(hist, bf), vm(tile_vals.shape, bf), vm(far, bf),
            vm((feat, feat), bf), vm((feat, feat), bf), vm(own, bf),
            vm((D, 1, slots), jnp.int32), vm((D, 1, slots), jnp.int32),
            vm((D, slots, slots), jnp.int32),
            vm(pulled, bf), vm(pulled, bf), vm(pulled, bf), vm(pulled, bf),
            vm((X * slots, feat), f32), vm(own, f32), vm(own, f32),
            vm(own, bf), vm(own, bf),
            vm((2, N // 2, piece, feat), f32), vm((N // 2, piece, feat), f32),
            vm((N // 2, piece, feat), f32),
            vm((piece, feat), bf), vm((N, piece, feat), bf),
            dma((11,)), pltpu.SemaphoreType.REGULAR((Z + X,)),
            dma((D,)), dma((D,)), dma((D,)), dma((D,)), dma((D,)), dma((D,)),
            dma((links, pieces)), dma((links, pieces)), dma, dma, dma, dma, dma, dma,
        ],
        compiler_params=pltpu.CompilerParams(
            collective_id=0, has_side_effects=True, vmem_limit_bytes=grant
        ),
    )(
        *[
            pltpu.with_memory_space_constraint(x, pltpu.HBM)
            for x in (
                tile_cols, pull_counts, pull_rows, h_zero.reshape(own), h_prev.reshape(own),
                hist_a.reshape(hist), hist_b.reshape(hist), tile_vals, weight_two, weight_three,
                grad_out.reshape(own),
            )
        ]
    )
    flat = (
        out3.reshape(h_zero.shape),
        fresh.reshape(R * h_zero.shape[0], feat),
        grad.reshape(feat, feat),
    )
    parts = (4, 8, 1)
    return pl.pallas_call(
        functools.partial(hand_over, parts),
        out_shape=tuple(jax.ShapeDtypeStruct(x.shape, x.dtype) for x in flat),
        in_specs=[vspec] * 3,
        out_specs=(any_spec,) * 3,
        scratch_shapes=[dma((sum(parts),))],
        compiler_params=pltpu.CompilerParams(vmem_limit_bytes=8 * 1024 * 1024),
    )(*flat)


def solution(mesh):
    both = ("dev", "rep")
    return jax.shard_map(
        functools.partial(local, mesh.shape["dev"], mesh.shape["rep"]),
        mesh=mesh,
        in_specs=(
            P(both, None), P(both, None), P("dev", None), P("dev", None),
            P(both, None, None, None), P(both, None), P(both, None, None), P(both, None),
            P(), P(), P(both, None),
        ),
        out_specs=(P(both, None), P("dev", None), P()),
        check_vma=False,
    )
```

```python
import functools
import math

import jax
import jax.numpy as jnp
from jax import lax
from jax.experimental import pallas as pl
from jax.experimental.pallas import tpu as pltpu
from jax.sharding import PartitionSpec as P

restart = 0.1
strength = 0.5
MESH = pl.DeviceIdType.MESH
scope = jax.named_scope


def kernel(
    D, R,
    cols_h, counts_h, rows_h,
    h_zero, h_prev, hist_a, hist_b, tile_vals, w_two, w_three, grad_out,
    layer_out, hist_out, grad_res,
    cols, counts, rows_in,
    zero_v, cur_v, hist_av, hist_bv, vals_v, far_v, w2_v, w3_v, up_v,
    ask, asked, hi, hot, send_a, send_b, pull_a, pull_b, acc_a, acc_b,
    fresh_v, low_v, g_send, g_recv, g_part, g_all,
    local_sem, stage_sem, idx_s, idx_r, a_s, a_r, b_s, b_r, f_s, f_r, g_s, g_r, p_s, p_r,
):
    N = D * R
    X = 2 if D % 2 == 0 else 1
    Z = D // X
    H = Z // 2
    d = lax.axis_index("dev")
    r = lax.axis_index("rep")
    z, x = lax.div(d, X), lax.rem(d, X)
    me = d * R + r
    slots = rows_in.shape[2]
    feat = hist_av.shape[2]
    blocks = vals_v.shape[0]
    tiles = vals_v.shape[1]
    home = 4
    home_blocks = hist_av.shape[0]
    far_base = blocks + home_blocks
    dense = tiles - home == D

    barrier = pltpu.get_barrier_semaphore()
    if R == 4:
        side = lax.rem(r, 2)
        mates = [r + 1 - 2 * side, lax.rem(r + 2, R)]
    else:
        side = lax.rem(r, 2)
        mates = [lax.rem(r + 1 + k, R) for k in range(R - 1)]

    def signal_dev(sem):
        for step in (1, -1):
            t = z + step

            @pl.when(jnp.logical_and(t >= 0, t < Z))
            def _():
                pl.semaphore_signal(sem, inc=1, device_id=(t * X + x, r), device_id_type=MESH)

        if X == 2:
            pl.semaphore_signal(sem, inc=1, device_id=(z * X + 1 - x, r), device_id_type=MESH)

    def wait_dev(sem, more):
        inner = lax.div(z + Z - 1, Z) + lax.div(2 * Z - 2 - z, Z)
        pl.semaphore_wait(sem, inner + X - 1 + more)

    def signal_rep(sem):
        for t in mates:
            pl.semaphore_signal(sem, inc=1, device_id=(d, t), device_id_type=MESH)

    signal_dev(barrier)
    signal_rep(barrier)

    loads = [
        (rows_h, rows_in), (counts_h, counts), (hist_a, hist_av), (tile_vals, vals_v), (cols_h, cols),
        (hist_b, hist_bv), (h_prev, cur_v), (h_zero, zero_v), (w_two, w2_v), (w_three, w3_v), (grad_out, up_v),
    ]
    copies = [pltpu.make_async_copy(s, t, local_sem.at[i]) for i, (s, t) in enumerate(loads)]
    for c in copies:
        c.start()

    def ask_peer(p):
        pltpu.make_async_remote_copy(
            src_ref=ask.at[p], dst_ref=asked.at[d], send_sem=idx_s, recv_sem=idx_r.at[d],
            device_id=(p, r), device_id_type=MESH,
        ).start()

    def ask_at(s):
        for step in (1, -1):
            t = z + step * (s + 1)

            @pl.when(jnp.logical_and(t >= 0, t < Z))
            def _():
                ask_peer(t * X + x)

            if X == 2:
                u = z + step * s
                ok = jnp.logical_and(u >= 0, u < Z)
                ok = jnp.logical_and(ok, s + (1 + step) > 0)

                @pl.when(ok)
                def _():
                    ask_peer(u * X + 1 - x)

    rounds = Z - 1 + X - 1
    lane = lax.broadcasted_iota(jnp.int32, (1, slots), 1)

    def mask_rows(p, _):
        ask[p] = jnp.where(lane < counts[0, p], rows_in[0, pl.ds(p, 1), :], -1)
        return 0

    def plane(m):
        if Z % 2:
            return lax.rem(z + 1 + m, Z)
        up = lax.div(z, H)
        over = (1 - up) * (H + m) + up * (H - 1 - m)
        near = up * H + lax.rem(z - up * H + 1 + m, H)
        far = lax.div(m, H)
        return (1 - far) * over + far * near

    span = X * slots
    bits = span.bit_length() - 1
    lanes = lax.broadcasted_iota(jnp.int32, (slots, slots), 1)
    low_width = span // slots

    def keys(q):
        @pl.when(q != d)
        def _():
            pltpu.make_async_remote_copy(
                src_ref=ask.at[q], dst_ref=asked.at[q], send_sem=idx_s, recv_sem=idx_r.at[q],
                device_id=(q, r), device_id_type=MESH,
            ).wait_recv()

        key = jnp.broadcast_to(asked[q], (slots, slots)).T
        hi[q] = lax.shift_right_arithmetic(key, bits).astype(jnp.float32).astype(jnp.bfloat16)
        rest = jnp.bitwise_and(key, span - 1)
        for w in range(low_width):
            hot[q, :, w * slots:(w + 1) * slots] = jnp.where(
                rest - w * slots == lanes, 1.0, 0.0
            ).astype(jnp.bfloat16)

    spans = home_blocks // low_width
    unit = 4

    def pick(table, base, count):
        tag = hi[pl.ds(base, count)].reshape(count * slots, slots)
        tag = jnp.concatenate([tag] * low_width, axis=1)
        low = hot[pl.ds(base, count)].reshape(count * slots, span)
        found = None
        for k in range(0, spans, unit):
            left = jnp.concatenate(
                [jnp.where(tag == jnp.bfloat16(k + u), low, jnp.bfloat16(0)) for u in range(unit)], axis=1
            )
            part = table[k * low_width:(k + unit) * low_width].reshape(unit * span, feat)
            got = jnp.dot(left, part, preferred_element_type=jnp.float32)
            found = got if found is None else found + got
        return found.astype(jnp.bfloat16).reshape(count, slots, feat)

    def serve(table, send_buf, pull_buf, s, q_sem, base, count):
        send_buf[pl.ds(base, count)] = pick(table, base, count)
        for e in range(count):
            q = base if count == 1 else base + lax.rem(x + 1 + e, count)

            @pl.when(q != d)
            def _():
                pltpu.make_async_remote_copy(
                    src_ref=send_buf.at[q], dst_ref=pull_buf.at[d], send_sem=s,
                    recv_sem=q_sem.at[z], device_id=(q, r), device_id_type=MESH,
                ).start()

    first = plane(0) * X

    def start_first():
        copies[2].wait()
        asked[d] = ask[d]
        q = first + x
        keys(q)
        serve(hist_av, send_a, pull_a, a_s, a_r, q, 1)

    beside = jnp.logical_or(z == H - 1, z == H)

    with scope("stages"):
        wait_dev(barrier, len(mates))
        signal_dev(stage_sem.at[0])
        copies[0].wait()
        copies[1].wait()
        if D <= 8:
            for p in range(D):
                mask_rows(p, 0)
        else:
            lax.fori_loop(0, D, mask_rows, 0)
        ask_at(0)

        def stage(s, _):
            wait_dev(stage_sem.at[s - 1], 0)

            @pl.when(s < rounds - 1)
            def _():
                signal_dev(stage_sem.at[s])

            ask_at(s)
            return 0

        for s in range(1, rounds) if rounds < 6 else ():
            if s == rounds - 1 and Z == 4:
                @pl.when(beside)
                def _():
                    start_first()
            stage(s, 0)
        if rounds >= 6:
            lax.fori_loop(1, rounds, stage, 0)
    signal_rep(stage_sem.at[rounds])

    def plane_copy(pull_buf, s, q_sem, zt, n):
        at = pull_buf.at[pl.ds(zt * X, n)]
        return pltpu.make_async_remote_copy(
            src_ref=at, dst_ref=at, send_sem=s, recv_sem=q_sem.at[zt],
            device_id=(lax.rem(d + 1, D), r), device_id_type=MESH,
        )

    def gather_a(m, _):
        base = plane(m) * X
        for e in range(X):
            keys(base + e)
        serve(hist_av, send_a, pull_a, a_s, a_r, base, X)
        return 0

    if Z == 4:
        turn = 2 * lax.rem(lax.div(z + 1, 2), 2)
    else:
        turn = 0

    def gather_b(m, _):
        k = lax.rem(m + turn, Z)
        if Z % 2 == 0:
            k = jnp.where(k < H, H - 1 - k, k)
        serve(hist_bv, send_b, pull_b, b_s, b_r, plane(k) * X, X)
        return 0

    with scope("gather_a"):
        if Z == 4 and rounds > 1:
            @pl.when(jnp.logical_not(beside))
            def _():
                start_first()
        else:
            start_first()
        for e in range(1, X):
            q = first + lax.rem(x + e, X)
            keys(q)
            serve(hist_av, send_a, pull_a, a_s, a_r, q, 1)
        lax.fori_loop(1, Z, gather_a, 0)
        pull_a[d] = send_a[d]

    pl.semaphore_wait(stage_sem.at[rounds], len(mates))
    if R == 4:
        signal_rep(stage_sem.at[rounds + 1])
    copies[5].wait()
    held = Z - H * lax.div(turn, H) if Z == 4 else Z
    with scope("gather_b"):
        lax.fori_loop(0, held, gather_b, 0)

    if dense:
        copies[3].wait()
        copies[4].wait()

        def spread_tiles(i, _):
            first = cols[i, home] - far_base
            for p in range(D):
                t = home + lax.rem(p - first + D, D)
                far_v[p // X, pl.ds(i * slots, slots), (p % X) * slots:(p % X + 1) * slots] = vals_v[i, t]
            return 0

        with scope("tiles"):
            lax.fori_loop(0, blocks, spread_tiles, 0)
    waited = (0, 1, 2, 3, 4, 5) if dense else (0, 1, 2, 5)
    for i in range(len(copies)):
        if i not in waited:
            copies[i].wait()

    def product(i, picks):
        left = jnp.concatenate([vals_v[i, t] for t, _ in picks], axis=1)
        right = jnp.concatenate([b for _, b in picks], axis=0)
        return jnp.dot(left, right, preferred_element_type=jnp.float32)

    def near_tiles(i, _):
        picks = [(0, cur_v[cols[i, 0]])]
        picks += [(t, hist_av[jnp.maximum(cols[i, t] - blocks, 0)]) for t in range(1, home)]
        acc_a[i] = product(i, picks)
        acc_b[i] = product(i, [(t, hist_bv[jnp.maximum(cols[i, t] - blocks, 0)]) for t in range(1, home)])
        return 0

    with scope("near"):
        lax.fori_loop(0, blocks, near_tiles, 0)
    with scope("gather_b2"):
        lax.fori_loop(held, Z, gather_b, 0)
        pull_b[d] = send_b[d]

    rows = blocks * slots

    def pull_plane(n, acc_ref, pull_buf, s, q_sem):
        if n == 0 or Z % 2:
            m = (n + Z - 1) % Z
        else:
            m = H + n - 1 if n < H else n - H
        zt = plane(m)
        if n == 0:
            if X > 1:
                plane_copy(pull_buf, s, q_sem, zt, X - 1).wait_recv()
        else:
            plane_copy(pull_buf, s, q_sem, zt, X).wait_recv()

        part = jnp.dot(
            far_v[zt], pull_buf[pl.ds(zt * X, X)].reshape(X * slots, feat),
            preferred_element_type=jnp.float32,
        )
        acc_ref[...] += part.reshape(blocks, slots, feat)

    def pull_all(acc_ref, pull_buf, s, q_sem):
        if dense:
            for n in range(Z):
                pull_plane(n, acc_ref, pull_buf, s, q_sem)
            return

        if X > 1:
            plane_copy(pull_buf, s, q_sem, z, X - 1).wait_recv()

        def one(k, _):
            plane_copy(pull_buf, s, q_sem, lax.rem(z + 1 + k, Z), X).wait_recv()
            return 0

        lax.fori_loop(0, Z - 1, one, 0)

        def far(i, _):
            acc_ref[i] += product(
                i, [(t, pull_buf[jnp.maximum(cols[i, t] - far_base, 0)]) for t in range(home, tiles)]
            )
            return 0

        lax.fori_loop(0, blocks, far, 0)

    factor_two = math.log(strength / 2 + 1.0)
    factor_three = math.log(strength / 3 + 1.0)

    def mix(acc_ref, at):
        return (1.0 - restart) * acc_ref[at] + restart * zero_v[at].astype(jnp.float32)

    def activate(mixed, low, w, factor):
        shape = mixed.shape
        prod = jnp.dot(low.reshape(-1, feat), w[...], preferred_element_type=jnp.float32)
        inner = (1.0 - factor) * mixed + factor * prod.reshape(shape)
        return jnp.maximum(inner, 0.0).astype(jnp.bfloat16)

    with scope("pull_a"):
        pull_all(acc_a, pull_a, a_s, a_r)

    step = 2 if blocks % 2 == 0 else 1
    pieces = blocks // step
    early = pieces - pieces // 4

    def fresh_copy(slot, target, k, c, n=1):
        at = pl.ds(c * step, n * step)
        recv = f_r.at[c] if k == 0 else f_r.at[pieces + k - 1]
        return pltpu.make_async_remote_copy(
            src_ref=hist_out.at[slot, at], dst_ref=hist_out.at[slot, at], send_sem=f_s.at[k],
            recv_sem=recv, device_id=(d, target), device_id_type=MESH,
        )

    if R == 4:
        mate, across = mates
        targets = [across, mate]
    else:
        mate, across = r + 1 - 2 * side, None
        targets = mates

    def second(c, _):
        at = pl.ds(c * step, step)
        mixed = mix(acc_a, at)
        made = activate(mixed, mixed.astype(jnp.bfloat16), w2_v, factor_two)
        fresh_v[at] = made
        hist_out[r, at] = made
        return 0

    with scope("second"):
        lax.fori_loop(0, pieces, second, 0)

        def send_fresh(c, _):
            for k, t in enumerate(targets):
                fresh_copy(r, t, k, c).start()
            return 0

        lax.fori_loop(0, early, send_fresh, 0)

    def own_tile(i, _):
        acc_b[i] += product(i, [(0, fresh_v[cols[i, 0]])])
        return 0

    with scope("own"):
        lax.fori_loop(0, blocks, own_tile, 0)

    with scope("pull_b"):
        pull_all(acc_b, pull_b, b_s, b_r)

    with scope("grad"):
        low_v[...] = mix(acc_b, slice(None)).astype(jnp.bfloat16)
        grad = factor_three * lax.dot_general(
            low_v[...].reshape(rows, feat), up_v[...].reshape(rows, feat),
            (((0,), (0,)), ((), ())), preferred_element_type=jnp.float32,
        )
        owners, piece = g_send.shape[:2]
        for c in range(owners):
            g_send[c] = grad[c * piece:(c + 1) * piece, :].astype(g_send.dtype)

    if R & (R - 1):
        def place(t):
            return lax.div(t, R), lax.rem(t, R)
    else:
        def place(t):
            return lax.shift_right_logical(t, R.bit_length() - 1), jnp.bitwise_and(t, R - 1)

    if owners < N:
        def reducer(o):
            return (H - 1) * X + lax.div(o, R // 2), 2 * lax.rem(o, R // 2) + 1

        own_part = (d - (H - 1) * X) * (R // 2) + lax.div(r, 2)
        reduces = jnp.logical_and(side == 1, jnp.logical_and(own_part >= 0, own_part < owners))
        turned = lax.div(owners, 2) * (1 - lax.div(z, H))
    else:
        reducer, own_part, reduces, turned = place, me, me >= 0, 0

    if R == 4:
        pl.semaphore_wait(stage_sem.at[rounds + 1], len(mates))

    def scatter(k, _):
        o = lax.rem(k + turned, owners)
        there = reducer(o)

        @pl.when(there[0] * R + there[1] != me)
        def _():
            pltpu.make_async_remote_copy(
                src_ref=g_send.at[o], dst_ref=g_recv.at[me], send_sem=g_s, recv_sem=g_r,
                device_id=there, device_id_type=MESH,
            ).start()

        return 0

    lax.fori_loop(0, owners, scatter, 0)
    lax.fori_loop(early, pieces, send_fresh, 0)

    def third(c, _):
        at = pl.ds(c * step, step)
        layer_out[at] = activate(mix(acc_b, at), low_v[at], w3_v, factor_three)
        return 0

    with scope("third"):
        lax.fori_loop(0, pieces, third, 0)

    def whole(ref, n, s, q):
        part = ref.at[pl.ds(0, n)]
        return pltpu.make_async_remote_copy(
            src_ref=part, dst_ref=part, send_sem=s, recv_sem=q,
            device_id=(lax.rem(d + 1, D), r), device_id_type=MESH,
        )

    @pl.when(reduces)
    def _():
        g_recv[me] = g_send[own_part]
        with scope("scatter"):
            whole(g_recv, N - 1, g_s, g_r).wait_recv()
        g_part[...] = jnp.sum(g_recv[...].astype(jnp.float32), axis=0).astype(g_part.dtype)

        def spread(k, _):
            t = k + jnp.where(k >= me, 1, 0)
            pltpu.make_async_remote_copy(
                src_ref=g_part, dst_ref=g_all.at[own_part], send_sem=p_s, recv_sem=p_r,
                device_id=place(t), device_id_type=MESH,
            ).start()
            return 0

        lax.fori_loop(0, N - 1, spread, 0)
        g_all[own_part] = g_part[...]

    if R == 4:
        def forward(c, _):
            fresh_copy(across, across, 0, c).wait_recv()
            fresh_copy(across, mate, 2, c).start()
            return 0

        with scope("forward"):
            lax.fori_loop(0, pieces, forward, 0)
    with scope("spread"):
        @pl.when(reduces)
        def _():
            whole(g_all, owners - 1, p_s, p_r).wait_recv()

        @pl.when(jnp.logical_not(reduces))
        def _():
            whole(g_all, owners, p_s, p_r).wait_recv()

    grad_res[...] = g_all[...].astype(jnp.float32)

    with scope("drain"):
        if R == 4:
            for k in (1, 2):
                fresh_copy(r, mate, k, 0, pieces).wait_recv()
        else:
            def landed(c, _):
                fresh_copy(r, mate, 0, c).wait_recv()
                return 0

            lax.fori_loop(0, pieces, landed, 0)
            for k in range(1, R - 1):
                fresh_copy(r, mate, k, 0, pieces).wait_recv()
        for k in range(3 if R == 4 else R - 1):
            fresh_copy(r, mate, k, 0, pieces).wait_send()
        whole(ask, D - 1, idx_s, p_r).wait_send()
        whole(send_a, D - 1, a_s, p_r).wait_send()
        whole(send_b, D - 1, b_s, p_r).wait_send()

        @pl.when(reduces)
        def _():
            whole(g_send, owners - 1, g_s, g_r).wait_send()
            whole(g_recv, N - 1, p_s, p_r).wait_send()

        @pl.when(jnp.logical_not(reduces))
        def _():
            whole(g_send, owners, g_s, g_r).wait_send()


def hand_over(parts, *refs):
    sources, targets, sem = refs[:3], refs[3:6], refs[6]
    outs = []
    for n, src, dst in zip(parts, sources, targets):
        rows = src.shape[0] // n
        for i in range(n):
            at = pl.ds(i * rows, rows)
            outs.append(pltpu.make_async_copy(src.at[at], dst.at[at], sem.at[len(outs)]))
    for c in outs:
        c.start()
    for c in outs:
        c.wait()


def local(D, R, h_zero, h_prev, hist_a, hist_b, tile_vals, tile_cols, pull_rows, pull_counts,
          weight_two, weight_three, grad_out):
    blocks, tiles, tile = tile_vals.shape[:3]
    feat = hist_a.shape[1]
    N = D * R
    hist_blocks = hist_a.shape[0] // tile
    bf, f32 = jnp.bfloat16, jnp.float32
    own = (blocks, tile, feat)
    hist = (hist_blocks, tile, feat)
    slots = pull_rows.shape[2]
    pulled = (D, slots, feat)
    X = 2 if D % 2 == 0 else 1
    Z = D // X
    dense = tiles - 4 == D
    owners = X * R if Z % 2 == 0 and R % 2 == 0 else N
    piece = feat // owners
    far = (Z, blocks * tile, X * tile) if dense else (1, 16, 128)
    pieces = blocks // 2 if blocks % 2 == 0 else blocks
    links = max(R - 1, 3)
    vm = pltpu.VMEM
    dma = pltpu.SemaphoreType.DMA
    any_spec = pl.BlockSpec(memory_space=pl.ANY)
    vspec = pl.BlockSpec(memory_space=pltpu.VMEM)
    grant = 24 * 2**20 + D * slots * (8 * feat + 8 * slots)
    out3, fresh, grad = pl.pallas_call(
        functools.partial(kernel, D, R),
        out_shape=(
            jax.ShapeDtypeStruct(own, bf),
            jax.ShapeDtypeStruct((R,) + own, bf),
            jax.ShapeDtypeStruct((owners, piece, feat), f32),
        ),
        in_specs=[any_spec] * 11,
        out_specs=(vspec, vspec, vspec),
        scratch_shapes=[
            pltpu.SMEM(tile_cols.shape, jnp.int32), pltpu.SMEM(pull_counts.shape, jnp.int32),
            vm(pull_rows.shape, jnp.int32),
            vm(own, bf), vm(own, bf), vm(hist, bf), vm(hist, bf), vm(tile_vals.shape, bf), vm(far, bf),
            vm((feat, feat), bf), vm((feat, feat), bf), vm(own, bf),
            vm((D, 1, slots), jnp.int32), vm((D, 1, slots), jnp.int32),
            vm((D, slots, slots), bf), vm((D, slots, X * slots), bf),
            vm(pulled, bf), vm(pulled, bf), vm(pulled, bf), vm(pulled, bf),
            vm(own, f32), vm(own, f32),
            vm(own, bf), vm(own, bf),
            vm((owners, piece, feat), bf), vm((N, piece, feat), bf),
            vm((piece, feat), bf), vm((owners, piece, feat), bf),
            dma((11,)), pltpu.SemaphoreType.REGULAR((Z + X,)),
            dma, dma((D,)), dma, dma((Z,)), dma, dma((Z,)),
            dma((links,)), dma((pieces + links - 1,)), dma, dma, dma, dma,
        ],
        compiler_params=pltpu.CompilerParams(
            collective_id=0, has_side_effects=True, vmem_limit_bytes=grant
        ),
    )(
        *[
            pltpu.with_memory_space_constraint(x, pltpu.HBM)
            for x in (
                tile_cols, pull_counts, pull_rows, h_zero.reshape(own), h_prev.reshape(own),
                hist_a.reshape(hist), hist_b.reshape(hist), tile_vals, weight_two, weight_three,
                grad_out.reshape(own),
            )
        ]
    )
    flat = (
        out3.reshape(h_zero.shape),
        fresh.reshape(R * h_zero.shape[0], feat),
        grad.reshape(feat, feat),
    )
    parts = (4, 8, 1)
    return pl.pallas_call(
        functools.partial(hand_over, parts),
        out_shape=tuple(jax.ShapeDtypeStruct(x.shape, x.dtype) for x in flat),
        in_specs=[vspec] * 3,
        out_specs=(any_spec,) * 3,
        scratch_shapes=[dma((sum(parts),))],
        compiler_params=pltpu.CompilerParams(vmem_limit_bytes=8 * 1024 * 1024),
    )(*flat)


def solution(mesh):
    both = ("dev", "rep")
    return jax.shard_map(
        functools.partial(local, mesh.shape["dev"], mesh.shape["rep"]),
        mesh=mesh,
        in_specs=(
            P(both, None), P(both, None), P("dev", None), P("dev", None),
            P(both, None, None, None), P(both, None), P(both, None, None), P(both, None),
            P(), P(), P(both, None),
        ),
        out_specs=(P(both, None), P("dev", None), P()),
        check_vma=False,
    )
```

```python
import functools
import math

import jax
import jax.numpy as jnp
from jax import lax
from jax.experimental import pallas as pl
from jax.experimental.pallas import tpu as pltpu
from jax.sharding import PartitionSpec as P

restart = 0.1
strength = 0.5
MESH = pl.DeviceIdType.MESH
scope = jax.named_scope


def kernel(
    D, R,
    cols_h, counts_h, rows_h,
    h_zero, h_prev, hist_a, hist_b, tile_vals, w_two, w_three, grad_out,
    layer_out, hist_out, grad_res,
    cols, counts, rows_in,
    zero_v, cur_v, hist_av, hist_bv, vals_v, far_v, w2_v, w3_v, up_v,
    ask, asked, hi, hot, send_a, send_b, pull_a, pull_b, acc_a, acc_b,
    fresh_v, low_v, g_term, g_mate, g_send, g_recv, g_part, g_all,
    local_sem, stage_sem, idx_s, idx_r, a_s, a_r, b_s, b_r, f_s, f_r, m_s, m_r, g_s, g_r, p_s, p_r,
):
    N = D * R
    X = 2 if D % 2 == 0 else 1
    Z = D // X
    H = Z // 2
    d = lax.axis_index("dev")
    r = lax.axis_index("rep")
    z, x = lax.div(d, X), lax.rem(d, X)
    me = d * R + r
    slots = rows_in.shape[2]
    feat = hist_av.shape[2]
    blocks = vals_v.shape[0]
    tiles = vals_v.shape[1]
    home = 4
    home_blocks = hist_av.shape[0]
    far_base = blocks + home_blocks
    dense = tiles - home == D

    barrier = pltpu.get_barrier_semaphore()
    if R == 4:
        side = lax.rem(r, 2)
        mates = [r + 1 - 2 * side, lax.rem(r + 2, R)]
    else:
        side = lax.rem(r, 2)
        mates = [lax.rem(r + 1 + k, R) for k in range(R - 1)]

    def signal_dev(sem):
        for step in (1, -1):
            t = z + step

            @pl.when(jnp.logical_and(t >= 0, t < Z))
            def _():
                pl.semaphore_signal(sem, inc=1, device_id=(t * X + x, r), device_id_type=MESH)

        if X == 2:
            pl.semaphore_signal(sem, inc=1, device_id=(z * X + 1 - x, r), device_id_type=MESH)

    def wait_dev(sem, more):
        inner = lax.div(z + Z - 1, Z) + lax.div(2 * Z - 2 - z, Z)
        pl.semaphore_wait(sem, inner + X - 1 + more)

    def signal_rep(sem):
        for t in mates:
            pl.semaphore_signal(sem, inc=1, device_id=(d, t), device_id_type=MESH)

    signal_dev(barrier)
    signal_rep(barrier)

    loads = [
        (rows_h, rows_in), (counts_h, counts), (hist_a, hist_av), (tile_vals, vals_v), (cols_h, cols),
        (hist_b, hist_bv), (h_prev, cur_v), (h_zero, zero_v), (w_two, w2_v), (w_three, w3_v), (grad_out, up_v),
    ]
    copies = [pltpu.make_async_copy(s, t, local_sem.at[i]) for i, (s, t) in enumerate(loads)]
    for c in copies:
        c.start()

    def ask_peer(p):
        pltpu.make_async_remote_copy(
            src_ref=ask.at[p], dst_ref=asked.at[d], send_sem=idx_s, recv_sem=idx_r.at[d],
            device_id=(p, r), device_id_type=MESH,
        ).start()

    def ask_at(s):
        for step in (1, -1):
            t = z + step * (s + 1)

            @pl.when(jnp.logical_and(t >= 0, t < Z))
            def _():
                ask_peer(t * X + x)

            if X == 2:
                u = z + step * s
                ok = jnp.logical_and(u >= 0, u < Z)
                ok = jnp.logical_and(ok, s + (1 + step) > 0)

                @pl.when(ok)
                def _():
                    ask_peer(u * X + 1 - x)

    rounds = Z - 1 + X - 1
    lane = lax.broadcasted_iota(jnp.int32, (1, slots), 1)

    def mask_rows(p, _):
        ask[p] = jnp.where(lane < counts[0, p], rows_in[0, pl.ds(p, 1), :], -1)
        return 0

    def plane(m):
        if Z % 2:
            return lax.rem(z + 1 + m, Z)
        up = lax.div(z, H)
        over = (1 - up) * (H + m) + up * (H - 1 - m)
        near = up * H + lax.rem(z - up * H + 1 + m, H)
        far = lax.div(m, H)
        return (1 - far) * over + far * near

    span = X * slots
    bits = span.bit_length() - 1
    lanes = lax.broadcasted_iota(jnp.int32, (slots, slots), 1)
    low_width = span // slots

    def keys(q):
        @pl.when(q != d)
        def _():
            pltpu.make_async_remote_copy(
                src_ref=ask.at[q], dst_ref=asked.at[q], send_sem=idx_s, recv_sem=idx_r.at[q],
                device_id=(q, r), device_id_type=MESH,
            ).wait_recv()

        key = jnp.broadcast_to(asked[q], (slots, slots)).T
        hi[q] = lax.shift_right_arithmetic(key, bits).astype(jnp.float32).astype(jnp.bfloat16)
        rest = jnp.bitwise_and(key, span - 1)
        for w in range(low_width):
            hot[q, :, w * slots:(w + 1) * slots] = jnp.where(
                rest - w * slots == lanes, 1.0, 0.0
            ).astype(jnp.bfloat16)

    spans = home_blocks // low_width
    unit = 4

    def pick(table, base, count):
        tag = hi[pl.ds(base, count)].reshape(count * slots, slots)
        tag = jnp.concatenate([tag] * low_width, axis=1)
        low = hot[pl.ds(base, count)].reshape(count * slots, span)
        found = None
        for k in range(0, spans, unit):
            left = jnp.concatenate(
                [jnp.where(tag == jnp.bfloat16(k + u), low, jnp.bfloat16(0)) for u in range(unit)], axis=1
            )
            part = table[k * low_width:(k + unit) * low_width].reshape(unit * span, feat)
            got = jnp.dot(left, part, preferred_element_type=jnp.float32)
            found = got if found is None else found + got
        return found.astype(jnp.bfloat16).reshape(count, slots, feat)

    def serve(table, send_buf, pull_buf, s, q_sem, base, count):
        send_buf[pl.ds(base, count)] = pick(table, base, count)
        ship(send_buf, pull_buf, s, q_sem, base, count)

    def ship(send_buf, pull_buf, s, q_sem, base, count):
        for e in range(count):
            q = base if count == 1 else base + lax.rem(x + 1 + e, count)

            @pl.when(q != d)
            def _():
                pltpu.make_async_remote_copy(
                    src_ref=send_buf.at[q], dst_ref=pull_buf.at[d], send_sem=s,
                    recv_sem=q_sem.at[z], device_id=(q, r), device_id_type=MESH,
                ).start()

    first = plane(0) * X

    def start_block(e):
        if e == 0:
            asked[d] = ask[d]
        q = first + lax.rem(x + e, X)
        keys(q)
        if e == 0:
            copies[2].wait()
        serve(hist_av, send_a, pull_a, a_s, a_r, q, 1)

    beside = jnp.logical_or(z == H - 1, z == H)

    with scope("stages"):
        wait_dev(barrier, len(mates))
        signal_dev(stage_sem.at[0])
        copies[0].wait()
        copies[1].wait()
        if D <= 8:
            for p in range(D):
                mask_rows(p, 0)
        else:
            lax.fori_loop(0, D, mask_rows, 0)
        ask_at(0)

        def stage(s, _):
            wait_dev(stage_sem.at[s - 1], 0)

            @pl.when(s < rounds - 1)
            def _():
                signal_dev(stage_sem.at[s])

            ask_at(s)
            return 0

        for s in range(1, rounds) if rounds < 6 else ():
            if Z == 4 and s >= 2:
                @pl.when(beside)
                def _():
                    start_block(s - 2)
            stage(s, 0)
        if rounds >= 6:
            lax.fori_loop(1, rounds, stage, 0)
    signal_rep(stage_sem.at[rounds])

    def plane_copy(pull_buf, s, q_sem, zt, n):
        at = pull_buf.at[pl.ds(zt * X, n)]
        return pltpu.make_async_remote_copy(
            src_ref=at, dst_ref=at, send_sem=s, recv_sem=q_sem.at[zt],
            device_id=(lax.rem(d + 1, D), r), device_id_type=MESH,
        )

    def gather_a(m, _):
        base = plane(m) * X
        for e in range(X):
            keys(base + e)
        serve(hist_av, send_a, pull_a, a_s, a_r, base, X)
        return 0

    if Z == 4:
        turn = 2 * lax.rem(lax.div(z + 1, 2), 2)
    else:
        turn = 0

    holds = beside if dense and Z == 4 else jnp.logical_and(side == 1, False)

    def gather_b(m, _):
        k = lax.rem(m + turn, Z)
        if Z % 2 == 0:
            k = jnp.where(k < H, H - 1 - k, k)
        base = plane(k) * X
        send_b[pl.ds(base, X)] = pick(hist_bv, base, X)

        @pl.when(jnp.logical_or(k >= H, jnp.logical_not(holds)))
        def _():
            ship(send_b, pull_b, b_s, b_r, base, X)

        return 0

    with scope("gather_a"):
        if Z == 4 and X == 2:
            @pl.when(jnp.logical_not(beside))
            def _():
                for e in range(X):
                    start_block(e)
        else:
            for e in range(X):
                start_block(e)
        lax.fori_loop(1, Z, gather_a, 0)
        pull_a[d] = send_a[d]

    pl.semaphore_wait(stage_sem.at[rounds], len(mates))
    if R == 4:
        signal_rep(stage_sem.at[rounds + 1])
    copies[5].wait()
    held = Z - H * lax.div(turn, H) if Z == 4 else Z
    with scope("gather_b"):
        lax.fori_loop(0, held, gather_b, 0)

    if dense:
        copies[3].wait()
        copies[4].wait()

        def spread_tiles(i, _):
            first = cols[i, home] - far_base
            for p in range(D):
                t = home + lax.rem(p - first + D, D)
                far_v[p // X, pl.ds(i * slots, slots), (p % X) * slots:(p % X + 1) * slots] = vals_v[i, t]
            return 0

        with scope("tiles"):
            lax.fori_loop(0, blocks, spread_tiles, 0)
    waited = (0, 1, 2, 3, 4, 5) if dense else (0, 1, 2, 5)
    for i in range(len(copies)):
        if i not in waited:
            copies[i].wait()

    def product(i, picks):
        left = jnp.concatenate([vals_v[i, t] for t, _ in picks], axis=1)
        right = jnp.concatenate([b for _, b in picks], axis=0)
        return jnp.dot(left, right, preferred_element_type=jnp.float32)

    def near_tiles(i, _):
        picks = [(0, cur_v[cols[i, 0]])]
        picks += [(t, hist_av[jnp.maximum(cols[i, t] - blocks, 0)]) for t in range(1, home)]
        acc_a[i] = product(i, picks)
        acc_b[i] = product(i, [(t, hist_bv[jnp.maximum(cols[i, t] - blocks, 0)]) for t in range(1, home)])
        return 0

    with scope("near"):
        lax.fori_loop(0, blocks, near_tiles, 0)
    with scope("gather_b2"):
        lax.fori_loop(held, Z, gather_b, 0)
        pull_b[d] = send_b[d]

    rows = blocks * slots

    def pull_plane(n, acc_ref, pull_buf, s, q_sem):
        if n == 0 or Z % 2:
            m = (n + Z - 1) % Z
        else:
            m = H + n - 1 if n < H else n - H
        zt = plane(m)
        if n == 0:
            if X > 1:
                plane_copy(pull_buf, s, q_sem, zt, X - 1).wait_recv()
        else:
            plane_copy(pull_buf, s, q_sem, zt, X).wait_recv()

        part = jnp.dot(
            far_v[zt], pull_buf[pl.ds(zt * X, X)].reshape(X * slots, feat),
            preferred_element_type=jnp.float32,
        )
        acc_ref[...] += part.reshape(blocks, slots, feat)

    def pull_all(acc_ref, pull_buf, s, q_sem):
        if dense:
            for n in range(Z):
                pull_plane(n, acc_ref, pull_buf, s, q_sem)
            return

        if X > 1:
            plane_copy(pull_buf, s, q_sem, z, X - 1).wait_recv()

        def one(k, _):
            plane_copy(pull_buf, s, q_sem, lax.rem(z + 1 + k, Z), X).wait_recv()
            return 0

        lax.fori_loop(0, Z - 1, one, 0)

        def far(i, _):
            acc_ref[i] += product(
                i, [(t, pull_buf[jnp.maximum(cols[i, t] - far_base, 0)]) for t in range(home, tiles)]
            )
            return 0

        lax.fori_loop(0, blocks, far, 0)

    factor_two = math.log(strength / 2 + 1.0)
    factor_three = math.log(strength / 3 + 1.0)

    def mix(acc_ref, at):
        return (1.0 - restart) * acc_ref[at] + restart * zero_v[at].astype(jnp.float32)

    def activate(mixed, low, w, factor):
        shape = mixed.shape
        prod = jnp.dot(low.reshape(-1, feat), w[...], preferred_element_type=jnp.float32)
        inner = (1.0 - factor) * mixed + factor * prod.reshape(shape)
        return jnp.maximum(inner, 0.0).astype(jnp.bfloat16)

    with scope("pull_a"):
        pull_all(acc_a, pull_a, a_s, a_r)

    if dense and Z == 4:
        @pl.when(holds)
        def _():
            for m in range(H):
                ship(send_b, pull_b, b_s, b_r, plane(H - 1 - m) * X, X)


    step = 2 if blocks % 2 == 0 else 1
    pieces = blocks // step
    early = pieces - pieces // 4

    def fresh_copy(slot, target, k, c, n=1):
        at = pl.ds(c * step, n * step)
        recv = f_r.at[c] if k == 0 else f_r.at[pieces + k - 1]
        return pltpu.make_async_remote_copy(
            src_ref=hist_out.at[slot, at], dst_ref=hist_out.at[slot, at], send_sem=f_s.at[k],
            recv_sem=recv, device_id=(d, target), device_id_type=MESH,
        )

    if R == 4:
        mate, across = mates
        targets = [across, mate]
    else:
        mate, across = r + 1 - 2 * side, None
        targets = mates

    def second(c, _):
        at = pl.ds(c * step, step)
        mixed = mix(acc_a, at)
        made = activate(mixed, mixed.astype(jnp.bfloat16), w2_v, factor_two)
        fresh_v[at] = made
        hist_out[r, at] = made
        return 0

    with scope("second"):
        lax.fori_loop(0, pieces, second, 0)

        def send_fresh(c, _):
            for k, t in enumerate(targets):
                fresh_copy(r, t, k, c).start()
            return 0

        lax.fori_loop(0, early, send_fresh, 0)

    def own_tile(i, _):
        acc_b[i] += product(i, [(0, fresh_v[cols[i, 0]])])
        return 0

    with scope("own"):
        lax.fori_loop(0, blocks, own_tile, 0)

    with scope("pull_b"):
        pull_all(acc_b, pull_b, b_s, b_r)

    with scope("grad"):
        low_v[...] = mix(acc_b, slice(None)).astype(jnp.bfloat16)
        grad = factor_three * lax.dot_general(
            low_v[...].reshape(rows, feat), up_v[...].reshape(rows, feat),
            (((0,), (0,)), ((), ())), preferred_element_type=jnp.float32,
        )
        owners, piece = g_send.shape[:2]
        g_term[...] = grad.reshape(owners, piece, feat)

    pair = r + 1 - 2 * side
    to_mate = pltpu.make_async_remote_copy(
        src_ref=g_term, dst_ref=g_mate, send_sem=m_s, recv_sem=m_r,
        device_id=(d, pair), device_id_type=MESH,
    )

    if R & (R - 1):
        def place(t):
            return lax.div(t, R), lax.rem(t, R)
    else:
        def place(t):
            return lax.shift_right_logical(t, R.bit_length() - 1), jnp.bitwise_and(t, R - 1)

    half = R // 2
    own_part = (d - (H - 1) * X) * half + lax.div(r, 2)
    reduces = jnp.logical_and(side == 1, jnp.logical_and(own_part >= 0, own_part < owners))
    turned = lax.div(owners, 2) * (1 - lax.div(z, H))
    voice = d * half + lax.div(r, 2)

    if R == 4:
        pl.semaphore_wait(stage_sem.at[rounds + 1], len(mates))

    @pl.when(side == 1)
    def _():
        to_mate.start()

    @pl.when(side == 0)
    def _():
        with scope("mate"):
            to_mate.wait_recv()
        g_send[...] = (g_term[...] + g_mate[...]).astype(g_send.dtype)

        def scatter(k, _):
            o = lax.rem(k + turned, owners)
            pltpu.make_async_remote_copy(
                src_ref=g_send.at[o], dst_ref=g_recv.at[voice], send_sem=g_s, recv_sem=g_r,
                device_id=((H - 1) * X + lax.div(o, half), 2 * lax.rem(o, half) + 1),
                device_id_type=MESH,
            ).start()
            return 0

        lax.fori_loop(0, owners, scatter, 0)

    lax.fori_loop(early, pieces, send_fresh, 0)

    def third(c, _):
        at = pl.ds(c * step, step)
        layer_out[at] = activate(mix(acc_b, at), low_v[at], w3_v, factor_three)
        return 0

    with scope("third"):
        lax.fori_loop(0, pieces, third, 0)

    def whole(ref, n, s, q):
        part = ref.at[pl.ds(0, n)]
        return pltpu.make_async_remote_copy(
            src_ref=part, dst_ref=part, send_sem=s, recv_sem=q,
            device_id=(lax.rem(d + 1, D), r), device_id_type=MESH,
        )

    @pl.when(reduces)
    def _():
        with scope("scatter"):
            whole(g_recv, N // 2, g_s, g_r).wait_recv()
        g_part[...] = jnp.sum(g_recv[...].astype(jnp.float32), axis=0).astype(g_part.dtype)

        def spread(k, _):
            t = k + jnp.where(k >= me, 1, 0)
            pltpu.make_async_remote_copy(
                src_ref=g_part, dst_ref=g_all.at[own_part], send_sem=p_s, recv_sem=p_r,
                device_id=place(t), device_id_type=MESH,
            ).start()
            return 0

        lax.fori_loop(0, N - 1, spread, 0)
        g_all[own_part] = g_part[...]

    if R == 4:
        def forward(c, _):
            fresh_copy(across, across, 0, c).wait_recv()
            fresh_copy(across, mate, 2, c).start()
            return 0

        with scope("forward"):
            lax.fori_loop(0, pieces, forward, 0)
    with scope("spread"):
        @pl.when(reduces)
        def _():
            whole(g_all, owners - 1, p_s, p_r).wait_recv()

        @pl.when(jnp.logical_not(reduces))
        def _():
            whole(g_all, owners, p_s, p_r).wait_recv()

    grad_res[...] = g_all[...].astype(jnp.float32)

    with scope("drain"):
        if R == 4:
            for k in (1, 2):
                fresh_copy(r, mate, k, 0, pieces).wait_recv()
        else:
            def landed(c, _):
                fresh_copy(r, mate, 0, c).wait_recv()
                return 0

            lax.fori_loop(0, pieces, landed, 0)
            for k in range(1, R - 1):
                fresh_copy(r, mate, k, 0, pieces).wait_recv()
        for k in range(3 if R == 4 else R - 1):
            fresh_copy(r, mate, k, 0, pieces).wait_send()
        whole(ask, D - 1, idx_s, p_r).wait_send()
        whole(send_a, D - 1, a_s, p_r).wait_send()
        whole(send_b, D - 1, b_s, p_r).wait_send()

        @pl.when(reduces)
        def _():
            def sent(k, _):
                pltpu.make_async_remote_copy(
                    src_ref=g_part, dst_ref=g_all.at[own_part], send_sem=p_s, recv_sem=p_r,
                    device_id=(d, pair), device_id_type=MESH,
                ).wait_send()
                return 0

            lax.fori_loop(0, N - 1, sent, 0)

        @pl.when(side == 1)
        def _():
            to_mate.wait_send()

        @pl.when(side == 0)
        def _():
            whole(g_send, owners, g_s, g_r).wait_send()


def hand_over(parts, *refs):
    sources, targets, sem = refs[:3], refs[3:6], refs[6]
    outs = []
    for n, src, dst in zip(parts, sources, targets):
        rows = src.shape[0] // n
        for i in range(n):
            at = pl.ds(i * rows, rows)
            outs.append(pltpu.make_async_copy(src.at[at], dst.at[at], sem.at[len(outs)]))
    for c in outs:
        c.start()
    for c in outs:
        c.wait()


def local(D, R, h_zero, h_prev, hist_a, hist_b, tile_vals, tile_cols, pull_rows, pull_counts,
          weight_two, weight_three, grad_out):
    blocks, tiles, tile = tile_vals.shape[:3]
    feat = hist_a.shape[1]
    N = D * R
    hist_blocks = hist_a.shape[0] // tile
    bf, f32 = jnp.bfloat16, jnp.float32
    own = (blocks, tile, feat)
    hist = (hist_blocks, tile, feat)
    slots = pull_rows.shape[2]
    pulled = (D, slots, feat)
    X = 2 if D % 2 == 0 else 1
    Z = D // X
    dense = tiles - 4 == D
    owners = X * R
    piece = feat // owners
    far = (Z, blocks * tile, X * tile) if dense else (1, 16, 128)
    pieces = blocks // 2 if blocks % 2 == 0 else blocks
    links = max(R - 1, 3)
    vm = pltpu.VMEM
    dma = pltpu.SemaphoreType.DMA
    any_spec = pl.BlockSpec(memory_space=pl.ANY)
    vspec = pl.BlockSpec(memory_space=pltpu.VMEM)
    grant = 24 * 2**20 + D * slots * (8 * feat + 8 * slots)
    out3, fresh, grad = pl.pallas_call(
        functools.partial(kernel, D, R),
        out_shape=(
            jax.ShapeDtypeStruct(own, bf),
            jax.ShapeDtypeStruct((R,) + own, bf),
            jax.ShapeDtypeStruct((owners, piece, feat), f32),
        ),
        in_specs=[any_spec] * 11,
        out_specs=(vspec, vspec, vspec),
        scratch_shapes=[
            pltpu.SMEM(tile_cols.shape, jnp.int32), pltpu.SMEM(pull_counts.shape, jnp.int32),
            vm(pull_rows.shape, jnp.int32),
            vm(own, bf), vm(own, bf), vm(hist, bf), vm(hist, bf), vm(tile_vals.shape, bf), vm(far, bf),
            vm((feat, feat), bf), vm((feat, feat), bf), vm(own, bf),
            vm((D, 1, slots), jnp.int32), vm((D, 1, slots), jnp.int32),
            vm((D, slots, slots), bf), vm((D, slots, X * slots), bf),
            vm(pulled, bf), vm(pulled, bf), vm(pulled, bf), vm(pulled, bf),
            vm(own, f32), vm(own, f32),
            vm(own, bf), vm(own, bf),
            vm((owners, piece, feat), f32), vm((owners, piece, feat), f32),
            vm((owners, piece, feat), bf), vm((N // 2, piece, feat), bf),
            vm((piece, feat), bf), vm((owners, piece, feat), bf),
            dma((11,)), pltpu.SemaphoreType.REGULAR((Z + X,)),
            dma, dma((D,)), dma, dma((Z,)), dma, dma((Z,)),
            dma((links,)), dma((pieces + links - 1,)), dma, dma, dma, dma, dma, dma,
        ],
        compiler_params=pltpu.CompilerParams(
            collective_id=0, has_side_effects=True, vmem_limit_bytes=grant
        ),
    )(
        *[
            pltpu.with_memory_space_constraint(x, pltpu.HBM)
            for x in (
                tile_cols, pull_counts, pull_rows, h_zero.reshape(own), h_prev.reshape(own),
                hist_a.reshape(hist), hist_b.reshape(hist), tile_vals, weight_two, weight_three,
                grad_out.reshape(own),
            )
        ]
    )
    flat = (
        out3.reshape(h_zero.shape),
        fresh.reshape(R * h_zero.shape[0], feat),
        grad.reshape(feat, feat),
    )
    parts = (4, 8, 1)
    return pl.pallas_call(
        functools.partial(hand_over, parts),
        out_shape=tuple(jax.ShapeDtypeStruct(x.shape, x.dtype) for x in flat),
        in_specs=[vspec] * 3,
        out_specs=(any_spec,) * 3,
        scratch_shapes=[dma((sum(parts),))],
        compiler_params=pltpu.CompilerParams(vmem_limit_bytes=8 * 1024 * 1024),
    )(*flat)


def solution(mesh):
    both = ("dev", "rep")
    return jax.shard_map(
        functools.partial(local, mesh.shape["dev"], mesh.shape["rep"]),
        mesh=mesh,
        in_specs=(
            P(both, None), P(both, None), P("dev", None), P("dev", None),
            P(both, None, None, None), P(both, None), P(both, None, None), P(both, None),
            P(), P(), P(both, None),
        ),
        out_specs=(P(both, None), P("dev", None), P()),
        check_vma=False,
    )
```

```python
import functools
import math

import jax
import jax.numpy as jnp
from jax import lax
from jax.experimental import pallas as pl
from jax.experimental.pallas import tpu as pltpu
from jax.sharding import PartitionSpec as P

restart = 0.1
strength = 0.5
MESH = pl.DeviceIdType.MESH
scope = jax.named_scope


def kernel(
    D, R,
    cols_h, counts_h, rows_h,
    h_zero, h_prev, hist_a, hist_b, tile_vals, w_two, w_three, grad_out,
    layer_out, hist_out, grad_res,
    cols, counts, rows_in,
    zero_v, cur_v, hist_av, hist_bv, vals_v, far_v, w2_v, w3_v, up_v,
    ask, asked, hi, hot, send_a, send_b, pull_a, pull_b, acc_a, acc_b,
    fresh_v, low_v, g_term, g_mate, g_send, g_recv, g_part, g_all,
    local_sem, stage_sem, idx_s, idx_r, a_s, a_r, b_s, b_r, f_s, f_r, g_s, g_r, p_s, p_r,
):
    N = D * R
    X = 2 if D % 2 == 0 else 1
    Z = D // X
    H = Z // 2
    d = lax.axis_index("dev")
    r = lax.axis_index("rep")
    z, x = lax.div(d, X), lax.rem(d, X)
    me = d * R + r
    slots = rows_in.shape[2]
    feat = hist_av.shape[2]
    blocks = vals_v.shape[0]
    tiles = vals_v.shape[1]
    home = 4
    home_blocks = hist_av.shape[0]
    far_base = blocks + home_blocks
    dense = tiles - home == D

    barrier = pltpu.get_barrier_semaphore()
    if R == 4:
        side = lax.rem(r, 2)
        mates = [r + 1 - 2 * side, lax.rem(r + 2, R)]
    else:
        side = lax.rem(r, 2)
        mates = [lax.rem(r + 1 + k, R) for k in range(R - 1)]

    def signal_dev(sem):
        for step in (1, -1):
            t = z + step

            @pl.when(jnp.logical_and(t >= 0, t < Z))
            def _():
                pl.semaphore_signal(sem, inc=1, device_id=(t * X + x, r), device_id_type=MESH)

        if X == 2:
            pl.semaphore_signal(sem, inc=1, device_id=(z * X + 1 - x, r), device_id_type=MESH)

    def wait_dev(sem, more):
        inner = lax.div(z + Z - 1, Z) + lax.div(2 * Z - 2 - z, Z)
        pl.semaphore_wait(sem, inner + X - 1 + more)

    def signal_rep(sem):
        for t in mates:
            pl.semaphore_signal(sem, inc=1, device_id=(d, t), device_id_type=MESH)

    signal_dev(barrier)
    signal_rep(barrier)

    loads = [
        (rows_h, rows_in), (counts_h, counts), (hist_a, hist_av), (tile_vals, vals_v), (cols_h, cols),
        (hist_b, hist_bv), (h_prev, cur_v), (h_zero, zero_v), (w_two, w2_v), (w_three, w3_v), (grad_out, up_v),
    ]
    prompt = 6
    copies = [pltpu.make_async_copy(s, t, local_sem.at[min(i, prompt)]) for i, (s, t) in enumerate(loads)]
    for c in copies:
        c.start()

    def ask_peer(p):
        pltpu.make_async_remote_copy(
            src_ref=ask.at[p], dst_ref=asked.at[d], send_sem=idx_s, recv_sem=idx_r.at[d],
            device_id=(p, r), device_id_type=MESH,
        ).start()

    def ask_at(s):
        for step in (1, -1):
            t = z + step * (s + 1)

            @pl.when(jnp.logical_and(t >= 0, t < Z))
            def _():
                ask_peer(t * X + x)

            if X == 2:
                u = z + step * s
                ok = jnp.logical_and(u >= 0, u < Z)
                ok = jnp.logical_and(ok, s + (1 + step) > 0)

                @pl.when(ok)
                def _():
                    ask_peer(u * X + 1 - x)

    rounds = Z - 1 + X - 1
    lane = lax.broadcasted_iota(jnp.int32, (1, slots), 1)

    def mask_rows(p, _):
        ask[p] = jnp.where(lane < counts[0, p], rows_in[0, pl.ds(p, 1), :], -1)
        return 0

    def plane(m):
        if Z % 2:
            return lax.rem(z + 1 + m, Z)
        up = lax.div(z, H)
        over = (1 - up) * (H + m) + up * (H - 1 - m)
        near = up * H + lax.rem(z - up * H + 1 + m, H)
        far = lax.div(m, H)
        return (1 - far) * over + far * near

    span = X * slots
    bits = span.bit_length() - 1
    lanes = lax.broadcasted_iota(jnp.int32, (slots, slots), 1)
    low_width = span // slots

    def keys(q):
        @pl.when(q != d)
        def _():
            pltpu.make_async_remote_copy(
                src_ref=ask.at[q], dst_ref=asked.at[q], send_sem=idx_s, recv_sem=idx_r.at[q],
                device_id=(q, r), device_id_type=MESH,
            ).wait_recv()

        key = jnp.broadcast_to(asked[q], (slots, slots)).T
        hi[q] = lax.shift_right_arithmetic(key, bits).astype(jnp.float32).astype(jnp.bfloat16)
        rest = jnp.bitwise_and(key, span - 1)
        for w in range(low_width):
            hot[q, :, w * slots:(w + 1) * slots] = jnp.where(
                rest - w * slots == lanes, 1.0, 0.0
            ).astype(jnp.bfloat16)

    spans = home_blocks // low_width
    unit = 4

    def pick(table, base, count):
        tag = hi[pl.ds(base, count)].reshape(count * slots, slots)
        tag = jnp.concatenate([tag] * low_width, axis=1)
        low = hot[pl.ds(base, count)].reshape(count * slots, span)
        found = None
        for k in range(0, spans, unit):
            left = jnp.concatenate(
                [jnp.where(tag == jnp.bfloat16(k + u), low, jnp.bfloat16(0)) for u in range(unit)], axis=1
            )
            part = table[k * low_width:(k + unit) * low_width].reshape(unit * span, feat)
            got = jnp.dot(left, part, preferred_element_type=jnp.float32)
            found = got if found is None else found + got
        return found.astype(jnp.bfloat16).reshape(count, slots, feat)

    def serve(table, send_buf, pull_buf, s, q_sem, base, count):
        send_buf[pl.ds(base, count)] = pick(table, base, count)
        ship(send_buf, pull_buf, s, q_sem, base, count)

    def ship(send_buf, pull_buf, s, q_sem, base, count):
        for e in range(count):
            q = base if count == 1 else base + lax.rem(x + 1 + e, count)

            @pl.when(q != d)
            def _():
                pltpu.make_async_remote_copy(
                    src_ref=send_buf.at[q], dst_ref=pull_buf.at[d], send_sem=s,
                    recv_sem=q_sem.at[z], device_id=(q, r), device_id_type=MESH,
                ).start()

    first = plane(0) * X

    def start_block(e):
        if e == 0:
            asked[d] = ask[d]
        q = first + lax.rem(x + e, X)
        keys(q)
        if e == 0:
            copies[2].wait()
        serve(hist_av, send_a, pull_a, a_s, a_r, q, 1)

    beside = jnp.logical_or(z == H - 1, z == H)

    with scope("stages"):
        wait_dev(barrier, len(mates))
        signal_dev(stage_sem.at[0])
        copies[0].wait()
        copies[1].wait()
        if D <= 8:
            for p in range(D):
                mask_rows(p, 0)
        else:
            lax.fori_loop(0, D, mask_rows, 0)
        ask_at(0)

        def stage(s, _):
            wait_dev(stage_sem.at[s - 1], 0)

            @pl.when(s < rounds - 1)
            def _():
                signal_dev(stage_sem.at[s])

            ask_at(s)
            return 0

        for s in range(1, rounds) if rounds < 6 else ():
            if Z == 4 and s >= 2:
                @pl.when(beside)
                def _():
                    start_block(s - 2)
            stage(s, 0)
        if rounds >= 6:
            lax.fori_loop(1, rounds, stage, 0)
    signal_rep(stage_sem.at[rounds - 1])

    def plane_copy(pull_buf, s, q_sem, zt, n):
        at = pull_buf.at[pl.ds(zt * X, n)]
        return pltpu.make_async_remote_copy(
            src_ref=at, dst_ref=at, send_sem=s, recv_sem=q_sem.at[zt],
            device_id=(lax.rem(d + 1, D), r), device_id_type=MESH,
        )

    def gather_a(m, _):
        base = plane(m) * X
        for e in range(X):
            keys(base + e)
        serve(hist_av, send_a, pull_a, a_s, a_r, base, X)
        return 0

    if Z == 4:
        turn = 2 * lax.rem(lax.div(z + 1, 2), 2)
    else:
        turn = 0

    holds = beside if dense and Z == 4 else jnp.logical_and(side == 1, False)

    def gather_b(m, _):
        k = lax.rem(m + turn, Z)
        if Z % 2 == 0:
            k = jnp.where(k < H, H - 1 - k, k)
        base = plane(k) * X
        send_b[pl.ds(base, X)] = pick(hist_bv, base, X)

        @pl.when(jnp.logical_or(k >= H, jnp.logical_not(holds)))
        def _():
            ship(send_b, pull_b, b_s, b_r, base, X)

        return 0

    with scope("gather_a"):
        if Z == 4 and X == 2:
            @pl.when(jnp.logical_not(beside))
            def _():
                for e in range(X):
                    start_block(e)
        else:
            for e in range(X):
                start_block(e)
        lax.fori_loop(1, Z, gather_a, 0)
        pull_a[d] = send_a[d]

    pl.semaphore_wait(stage_sem.at[rounds - 1], len(mates))
    if R == 4:
        signal_rep(stage_sem.at[rounds])
    copies[5].wait()
    held = Z - H * lax.div(turn, H) if Z == 4 else Z
    with scope("gather_b"):
        lax.fori_loop(0, held, gather_b, 0)

    if dense:
        copies[3].wait()
        copies[4].wait()

        def spread_tiles(i, _):
            first = cols[i, home] - far_base
            for p in range(D):
                t = home + lax.rem(p - first + D, D)
                far_v[p // X, pl.ds(i * slots, slots), (p % X) * slots:(p % X + 1) * slots] = vals_v[i, t]
            return 0

        with scope("tiles"):
            lax.fori_loop(0, blocks, spread_tiles, 0)
    if not dense:
        copies[3].wait()
        copies[4].wait()
    late_bytes = sum(math.prod(t.shape) for _, t in loads[prompt:])
    span_all = pl.ds(0, late_bytes // (slots * feat))
    pltpu.make_async_copy(hist_a.at[span_all], hist_av.at[span_all], local_sem.at[prompt]).wait()

    def product(i, picks):
        left = jnp.concatenate([vals_v[i, t] for t, _ in picks], axis=1)
        right = jnp.concatenate([b for _, b in picks], axis=0)
        return jnp.dot(left, right, preferred_element_type=jnp.float32)

    def near_tiles(i, _):
        picks = [(0, cur_v[cols[i, 0]])]
        picks += [(t, hist_av[jnp.maximum(cols[i, t] - blocks, 0)]) for t in range(1, home)]
        acc_a[i] = product(i, picks)
        acc_b[i] = product(i, [(t, hist_bv[jnp.maximum(cols[i, t] - blocks, 0)]) for t in range(1, home)])
        return 0

    with scope("near"):
        lax.fori_loop(0, blocks, near_tiles, 0)
    with scope("gather_b2"):
        lax.fori_loop(held, Z, gather_b, 0)
        pull_b[d] = send_b[d]

    rows = blocks * slots

    def arrive(n, pull_buf, s, q_sem):
        if n == 0 or Z % 2:
            m = (n + Z - 1) % Z
        else:
            m = H + n - 1 if n < H else n - H
        zt = plane(m)
        if n == 0:
            if X > 1:
                plane_copy(pull_buf, s, q_sem, zt, X - 1).wait_recv()
        else:
            plane_copy(pull_buf, s, q_sem, zt, X).wait_recv()

        return zt

    def pull_plane(n, acc_ref, pull_buf, s, q_sem):
        zt = arrive(n, pull_buf, s, q_sem)
        part = jnp.dot(
            far_v[zt], pull_buf[pl.ds(zt * X, X)].reshape(X * slots, feat),
            preferred_element_type=jnp.float32,
        )
        acc_ref[...] += part.reshape(blocks, slots, feat)

    def pull_all(acc_ref, pull_buf, s, q_sem, count=Z):
        if dense:
            for n in range(count):
                pull_plane(n, acc_ref, pull_buf, s, q_sem)
            return

        if X > 1:
            plane_copy(pull_buf, s, q_sem, z, X - 1).wait_recv()

        def one(k, _):
            plane_copy(pull_buf, s, q_sem, lax.rem(z + 1 + k, Z), X).wait_recv()
            return 0

        lax.fori_loop(0, Z - 1, one, 0)

        def far(i, _):
            acc_ref[i] += product(
                i, [(t, pull_buf[jnp.maximum(cols[i, t] - far_base, 0)]) for t in range(home, tiles)]
            )
            return 0

        lax.fori_loop(0, blocks, far, 0)

    factor_two = math.log(strength / 2 + 1.0)
    factor_three = math.log(strength / 3 + 1.0)

    def mix(acc_ref, at):
        return (1.0 - restart) * acc_ref[at] + restart * zero_v[at].astype(jnp.float32)

    def activate(mixed, low, w, factor):
        shape = mixed.shape
        prod = jnp.dot(low.reshape(-1, feat), w[...], preferred_element_type=jnp.float32)
        inner = (1.0 - factor) * mixed + factor * prod.reshape(shape)
        return jnp.maximum(inner, 0.0).astype(jnp.bfloat16)

    with scope("pull_a"):
        pull_all(acc_a, pull_a, a_s, a_r)

    if dense and Z == 4:
        @pl.when(holds)
        def _():
            for m in range(H):
                ship(send_b, pull_b, b_s, b_r, plane(H - 1 - m) * X, X)


    step = 2 if blocks % 2 == 0 else 1
    pieces = blocks // step
    early = pieces

    def fresh_copy(slot, target, k, c, n=1):
        at = pl.ds(c * step, n * step)
        recv = f_r.at[c] if k == 0 else f_r.at[pieces + k - 1]
        return pltpu.make_async_remote_copy(
            src_ref=hist_out.at[slot, at], dst_ref=hist_out.at[slot, at], send_sem=f_s,
            recv_sem=recv, device_id=(d, target), device_id_type=MESH,
        )

    if R == 4:
        mate, across = mates
        targets = [across, mate]
    else:
        mate, across = r + 1 - 2 * side, None
        targets = mates

    def second(c, _):
        at = pl.ds(c * step, step)
        mixed = mix(acc_a, at)
        made = activate(mixed, mixed.astype(jnp.bfloat16), w2_v, factor_two)
        fresh_v[at] = made
        hist_out[r, at] = made
        return 0

    with scope("second"):
        lax.fori_loop(0, pieces, second, 0)

        def send_fresh(c, _):
            for k, t in enumerate(targets):
                fresh_copy(r, t, k, c).start()
            return 0

        lax.fori_loop(0, early, send_fresh, 0)

    def own_tile(i, _):
        acc_b[i] += product(i, [(0, fresh_v[cols[i, 0]])])
        return 0

    with scope("own"):
        lax.fori_loop(0, blocks, own_tile, 0)

    with scope("pull_b"):
        pull_all(acc_b, pull_b, b_s, b_r, Z - 1)
        acc_b[...] = mix(acc_b, slice(None))
        last = arrive(Z - 1, pull_b, b_s, b_r) if dense else None
    with scope("grad"):
        mixed = acc_b[...].reshape(rows, feat)
        if dense:
            late = pull_b[pl.ds(last * X, X)].reshape(X * slots, feat)
            part = jnp.dot(far_v[last], late, preferred_element_type=jnp.float32)
            mixed = mixed + (1.0 - restart) * part
            acc_b[...] = mixed.reshape(blocks, slots, feat)
        low = mixed.astype(jnp.bfloat16)
        low_v[...] = low.reshape(blocks, slots, feat)
        grad = factor_three * lax.dot_general(
            low, up_v[...].reshape(rows, feat),
            (((0,), (0,)), ((), ())), preferred_element_type=jnp.float32,
        )
        owners, piece = g_send.shape[:2]
        g_term[...] = grad.reshape(owners, piece, feat)

    pair = r + 1 - 2 * side
    to_mate = pltpu.make_async_remote_copy(
        src_ref=g_term, dst_ref=g_mate, send_sem=g_s, recv_sem=g_r,
        device_id=(d, pair), device_id_type=MESH,
    )

    if R & (R - 1):
        def place(t):
            return lax.div(t, R), lax.rem(t, R)
    else:
        def place(t):
            return lax.shift_right_logical(t, R.bit_length() - 1), jnp.bitwise_and(t, R - 1)

    half = R // 2
    own_part = (d - (H - 1) * X) * half + lax.div(r, 2)
    reduces = jnp.logical_and(side == 1, jnp.logical_and(own_part >= 0, own_part < owners))
    turned = lax.div(owners, 2) * (1 - lax.div(z, H))
    voice = d * half + lax.div(r, 2)

    if R == 4:
        pl.semaphore_wait(stage_sem.at[rounds], len(mates))

    @pl.when(side == 1)
    def _():
        to_mate.start()

    @pl.when(side == 0)
    def _():
        with scope("mate"):
            to_mate.wait_recv()
        g_send[...] = (g_term[...] + g_mate[...]).astype(g_send.dtype)

        def scatter(k, _):
            o = lax.rem(k + turned, owners)
            pltpu.make_async_remote_copy(
                src_ref=g_send.at[o], dst_ref=g_recv.at[voice], send_sem=g_s, recv_sem=g_r,
                device_id=((H - 1) * X + lax.div(o, half), 2 * lax.rem(o, half) + 1),
                device_id_type=MESH,
            ).start()
            return 0

        lax.fori_loop(0, owners, scatter, 0)

    lax.fori_loop(early, pieces, send_fresh, 0)

    def third(c, _):
        at = pl.ds(c * step, step)
        layer_out[at] = activate(acc_b[at], low_v[at], w3_v, factor_three)
        return 0

    with scope("third"):
        lax.fori_loop(0, pieces, third, 0)

    def whole(ref, n, s, q):
        part = ref.at[pl.ds(0, n)]
        return pltpu.make_async_remote_copy(
            src_ref=part, dst_ref=part, send_sem=s, recv_sem=q,
            device_id=(lax.rem(d + 1, D), r), device_id_type=MESH,
        )

    @pl.when(reduces)
    def _():
        with scope("scatter"):
            whole(g_recv, N // 2, g_s, g_r).wait_recv()
        g_part[...] = jnp.sum(g_recv[...].astype(jnp.float32), axis=0).astype(g_part.dtype)

        def spread(k, _):
            t = k + jnp.where(k >= me, 1, 0)
            pltpu.make_async_remote_copy(
                src_ref=g_part, dst_ref=g_all.at[own_part], send_sem=p_s, recv_sem=p_r,
                device_id=place(t), device_id_type=MESH,
            ).start()
            return 0

        lax.fori_loop(0, N - 1, spread, 0)
        g_all[own_part] = g_part[...]

    if R == 4:
        def forward(c, _):
            fresh_copy(across, across, 0, c).wait_recv()
            fresh_copy(across, mate, 2, c).start()
            return 0

        with scope("forward"):
            lax.fori_loop(0, pieces, forward, 0)
    with scope("spread"):
        @pl.when(reduces)
        def _():
            whole(g_all, owners - 1, p_s, p_r).wait_recv()

        @pl.when(jnp.logical_not(reduces))
        def _():
            whole(g_all, owners, p_s, p_r).wait_recv()

    grad_res[...] = g_all[...].astype(jnp.float32)

    with scope("drain"):
        if R == 4:
            for k in (1, 2):
                fresh_copy(r, mate, k, 0, pieces).wait_recv()
        else:
            def landed(c, _):
                fresh_copy(r, mate, 0, c).wait_recv()
                return 0

            lax.fori_loop(0, pieces, landed, 0)
            for k in range(1, R - 1):
                fresh_copy(r, mate, k, 0, pieces).wait_recv()
        whole(hist_out, R - 1, f_s, p_r).wait_send()
        whole(ask, D - 1, idx_s, p_r).wait_send()
        whole(send_a, D - 1, a_s, p_r).wait_send()
        whole(send_b, D - 1, b_s, p_r).wait_send()

        @pl.when(reduces)
        def _():
            def sent(k, _):
                pltpu.make_async_remote_copy(
                    src_ref=g_part, dst_ref=g_all.at[own_part], send_sem=p_s, recv_sem=p_r,
                    device_id=(d, pair), device_id_type=MESH,
                ).wait_send()
                return 0

            lax.fori_loop(0, N - 1, sent, 0)

        @pl.when(side == 1)
        def _():
            to_mate.wait_send()

        @pl.when(side == 0)
        def _():
            whole(g_send, owners, g_s, g_r).wait_send()


def hand_over(parts, *refs):
    sources, targets, sem = refs[:3], refs[3:6], refs[6]
    outs = []
    for n, src, dst in zip(parts, sources, targets):
        rows = src.shape[0] // n
        for i in range(n):
            at = pl.ds(i * rows, rows)
            outs.append(pltpu.make_async_copy(src.at[at], dst.at[at], sem.at[len(outs)]))
    for c in outs:
        c.start()
    for c in outs:
        c.wait()


def local(D, R, h_zero, h_prev, hist_a, hist_b, tile_vals, tile_cols, pull_rows, pull_counts,
          weight_two, weight_three, grad_out):
    blocks, tiles, tile = tile_vals.shape[:3]
    feat = hist_a.shape[1]
    N = D * R
    hist_blocks = hist_a.shape[0] // tile
    bf, f32 = jnp.bfloat16, jnp.float32
    own = (blocks, tile, feat)
    hist = (hist_blocks, tile, feat)
    slots = pull_rows.shape[2]
    pulled = (D, slots, feat)
    X = 2 if D % 2 == 0 else 1
    Z = D // X
    dense = tiles - 4 == D
    owners = X * R
    piece = feat // owners
    far = (Z, blocks * tile, X * tile) if dense else (1, 16, 128)
    pieces = blocks // 2 if blocks % 2 == 0 else blocks
    links = max(R - 1, 3)
    vm = pltpu.VMEM
    dma = pltpu.SemaphoreType.DMA
    any_spec = pl.BlockSpec(memory_space=pl.ANY)
    vspec = pl.BlockSpec(memory_space=pltpu.VMEM)
    grant = 24 * 2**20 + D * slots * (8 * feat + 8 * slots)
    out3, fresh, grad = pl.pallas_call(
        functools.partial(kernel, D, R),
        out_shape=(
            jax.ShapeDtypeStruct(own, bf),
            jax.ShapeDtypeStruct((R,) + own, bf),
            jax.ShapeDtypeStruct((owners, piece, feat), f32),
        ),
        in_specs=[any_spec] * 11,
        out_specs=(vspec, vspec, vspec),
        scratch_shapes=[
            pltpu.SMEM(tile_cols.shape, jnp.int32), pltpu.SMEM(pull_counts.shape, jnp.int32),
            vm(pull_rows.shape, jnp.int32),
            vm(own, bf), vm(own, bf), vm(hist, bf), vm(hist, bf), vm(tile_vals.shape, bf), vm(far, bf),
            vm((feat, feat), bf), vm((feat, feat), bf), vm(own, bf),
            vm((D, 1, slots), jnp.int32), vm((D, 1, slots), jnp.int32),
            vm((D, slots, slots), bf), vm((D, slots, X * slots), bf),
            vm(pulled, bf), vm(pulled, bf), vm(pulled, bf), vm(pulled, bf),
            vm(own, f32), vm(own, f32),
            vm(own, bf), vm(own, bf),
            vm((owners, piece, feat), f32), vm((owners, piece, feat), f32),
            vm((owners, piece, feat), bf), vm((N // 2, piece, feat), bf),
            vm((piece, feat), bf), vm((owners, piece, feat), bf),
            dma((7,)), pltpu.SemaphoreType.REGULAR((Z + X - 1,)),
            dma, dma((D,)), dma, dma((Z,)), dma, dma((Z,)),
            dma, dma((pieces + links - 1,)), dma, dma, dma, dma,
        ],
        compiler_params=pltpu.CompilerParams(
            collective_id=0, has_side_effects=True, vmem_limit_bytes=grant
        ),
    )(
        *[
            pltpu.with_memory_space_constraint(x, pltpu.HBM)
            for x in (
                tile_cols, pull_counts, pull_rows, h_zero.reshape(own), h_prev.reshape(own),
                hist_a.reshape(hist), hist_b.reshape(hist), tile_vals, weight_two, weight_three,
                grad_out.reshape(own),
            )
        ]
    )
    flat = (
        out3.reshape(h_zero.shape),
        fresh.reshape(R * h_zero.shape[0], feat),
        grad.reshape(feat, feat),
    )
    parts = (1, 1, 1)
    return pl.pallas_call(
        functools.partial(hand_over, parts),
        out_shape=tuple(jax.ShapeDtypeStruct(x.shape, x.dtype) for x in flat),
        in_specs=[vspec] * 3,
        out_specs=(any_spec,) * 3,
        scratch_shapes=[dma((sum(parts),))],
        compiler_params=pltpu.CompilerParams(vmem_limit_bytes=8 * 1024 * 1024),
    )(*flat)


def solution(mesh):
    both = ("dev", "rep")
    return jax.shard_map(
        functools.partial(local, mesh.shape["dev"], mesh.shape["rep"]),
        mesh=mesh,
        in_specs=(
            P(both, None), P(both, None), P("dev", None), P("dev", None),
            P(both, None, None, None), P(both, None), P(both, None, None), P(both, None),
            P(), P(), P(both, None),
        ),
        out_specs=(P(both, None), P("dev", None), P()),
        check_vma=False,
    )
```

```python
import functools
import math

import jax
import jax.numpy as jnp
from jax import lax
from jax.experimental import pallas as pl
from jax.experimental.pallas import tpu as pltpu
from jax.sharding import PartitionSpec as P

restart = 0.1
strength = 0.5
MESH = pl.DeviceIdType.MESH
scope = jax.named_scope


def kernel(
    D, R,
    cols_h, counts_h, rows_h,
    h_zero, h_prev, hist_a, hist_b, tile_vals, w_two, w_three, grad_out,
    layer_out, hist_out, grad_res,
    cols, counts, rows_in,
    zero_v, cur_v, hist_av, hist_bv, vals_v, far_v, w2_v, w3_v, up_v,
    ask, asked, hi, hot, send_a, send_b, pull_a, pull_b, acc_a, acc_b,
    fresh_v, low_v, g_term, g_mate, g_send, g_recv, g_part, g_all,
    local_sem, stage_sem, idx_s, idx_r, a_s, a_r, b_s, b_r, f_s, f_r, g_s, g_r, p_s, p_r,
):
    N = D * R
    X = 2 if D % 2 == 0 else 1
    Z = D // X
    H = Z // 2
    d = lax.axis_index("dev")
    r = lax.axis_index("rep")
    z, x = lax.div(d, X), lax.rem(d, X)
    me = d * R + r
    slots = rows_in.shape[2]
    feat = hist_av.shape[2]
    blocks = vals_v.shape[0]
    tiles = vals_v.shape[1]
    home = 4
    home_blocks = hist_av.shape[0]
    far_base = blocks + home_blocks
    dense = tiles - home == D

    barrier = pltpu.get_barrier_semaphore()
    if R == 4:
        side = lax.rem(r, 2)
        mates = [r + 1 - 2 * side, lax.rem(r + 2, R)]
    else:
        side = lax.rem(r, 2)
        mates = [lax.rem(r + 1 + k, R) for k in range(R - 1)]

    def signal_dev(sem):
        for step in (1, -1):
            t = z + step

            @pl.when(jnp.logical_and(t >= 0, t < Z))
            def _():
                pl.semaphore_signal(sem, inc=1, device_id=(t * X + x, r), device_id_type=MESH)

        if X == 2:
            pl.semaphore_signal(sem, inc=1, device_id=(z * X + 1 - x, r), device_id_type=MESH)

    def wait_dev(sem, more):
        inner = lax.div(z + Z - 1, Z) + lax.div(2 * Z - 2 - z, Z)
        pl.semaphore_wait(sem, inner + X - 1 + more)

    def signal_rep(sem):
        for t in mates:
            pl.semaphore_signal(sem, inc=1, device_id=(d, t), device_id_type=MESH)

    signal_dev(barrier)
    signal_rep(barrier)

    loads = [
        (rows_h, rows_in), (counts_h, counts), (hist_a, hist_av), (tile_vals, vals_v), (cols_h, cols),
        (hist_b, hist_bv), (h_prev, cur_v), (h_zero, zero_v), (w_two, w2_v), (w_three, w3_v), (grad_out, up_v),
    ]
    prompt = 6
    copies = [pltpu.make_async_copy(s, t, local_sem.at[min(i, prompt)]) for i, (s, t) in enumerate(loads)]
    for c in copies:
        c.start()

    def ask_peer(p):
        pltpu.make_async_remote_copy(
            src_ref=ask.at[p], dst_ref=asked.at[d], send_sem=idx_s, recv_sem=idx_r.at[d],
            device_id=(p, r), device_id_type=MESH,
        ).start()

    def ask_at(s):
        for step in (1, -1):
            t = z + step * (s + 1)

            @pl.when(jnp.logical_and(t >= 0, t < Z))
            def _():
                ask_peer(t * X + x)

            if X == 2:
                u = z + step * s
                ok = jnp.logical_and(u >= 0, u < Z)
                ok = jnp.logical_and(ok, s + (1 + step) > 0)

                @pl.when(ok)
                def _():
                    ask_peer(u * X + 1 - x)

    rounds = Z - 1 + X - 1
    lane = lax.broadcasted_iota(jnp.int32, (1, slots), 1)

    def mask_rows(p, _):
        ask[p] = jnp.where(lane < counts[0, p], rows_in[0, pl.ds(p, 1), :], -1)
        return 0

    def plane(m):
        if Z % 2:
            return lax.rem(z + 1 + m, Z)
        up = lax.div(z, H)
        over = (1 - up) * (H + m) + up * (H - 1 - m)
        near = up * H + lax.rem(z - up * H + 1 + m, H)
        far = lax.div(m, H)
        return (1 - far) * over + far * near

    span = X * slots
    bits = span.bit_length() - 1
    lanes = lax.broadcasted_iota(jnp.int32, (slots, slots), 1)
    low_width = span // slots

    def keys(q):
        @pl.when(q != d)
        def _():
            pltpu.make_async_remote_copy(
                src_ref=ask.at[q], dst_ref=asked.at[q], send_sem=idx_s, recv_sem=idx_r.at[q],
                device_id=(q, r), device_id_type=MESH,
            ).wait_recv()

        key = jnp.broadcast_to(asked[q], (slots, slots)).T
        hi[q] = lax.shift_right_arithmetic(key, bits).astype(jnp.float32).astype(jnp.bfloat16)
        rest = jnp.bitwise_and(key, span - 1)
        for w in range(low_width):
            hot[q, :, w * slots:(w + 1) * slots] = jnp.where(
                rest - w * slots == lanes, 1.0, 0.0
            ).astype(jnp.bfloat16)

    spans = home_blocks // low_width
    unit = 4

    def pick(table, base, count):
        tag = hi[pl.ds(base, count)].reshape(count * slots, slots)
        tag = jnp.concatenate([tag] * low_width, axis=1)
        low = hot[pl.ds(base, count)].reshape(count * slots, span)
        found = None
        for k in range(0, spans, unit):
            left = jnp.concatenate(
                [jnp.where(tag == jnp.bfloat16(k + u), low, jnp.bfloat16(0)) for u in range(unit)], axis=1
            )
            part = table[k * low_width:(k + unit) * low_width].reshape(unit * span, feat)
            got = jnp.dot(left, part, preferred_element_type=jnp.float32)
            found = got if found is None else found + got
        return found.astype(jnp.bfloat16).reshape(count, slots, feat)

    def serve(table, send_buf, pull_buf, s, q_sem, base, count):
        send_buf[pl.ds(base, count)] = pick(table, base, count)
        ship(send_buf, pull_buf, s, q_sem, base, count)

    def ship(send_buf, pull_buf, s, q_sem, base, count):
        for e in range(count):
            q = base if count == 1 else base + lax.rem(x + 1 + e, count)

            @pl.when(q != d)
            def _():
                pltpu.make_async_remote_copy(
                    src_ref=send_buf.at[q], dst_ref=pull_buf.at[d], send_sem=s,
                    recv_sem=q_sem.at[z], device_id=(q, r), device_id_type=MESH,
                ).start()

    first = plane(0) * X

    def start_block(e):
        if e == 0:
            asked[d] = ask[d]
        q = first + lax.rem(x + e, X)
        keys(q)
        if e == 0:
            copies[2].wait()
        serve(hist_av, send_a, pull_a, a_s, a_r, q, 1)

    beside = jnp.logical_or(z == H - 1, z == H)

    with scope("stages"):
        wait_dev(barrier, len(mates))
        signal_dev(stage_sem.at[0])
        copies[0].wait()
        copies[1].wait()
        if D <= 8:
            for p in range(D):
                mask_rows(p, 0)
        else:
            lax.fori_loop(0, D, mask_rows, 0)
        ask_at(0)

        def stage(s, _):
            wait_dev(stage_sem.at[s - 1], 0)

            @pl.when(s < rounds - 1)
            def _():
                signal_dev(stage_sem.at[s])

            ask_at(s)
            return 0

        for s in range(1, rounds) if rounds < 6 else ():
            if Z == 4 and s >= 2:
                @pl.when(beside)
                def _():
                    start_block(s - 2)
            stage(s, 0)
        if rounds >= 6:
            lax.fori_loop(1, rounds, stage, 0)
    signal_rep(stage_sem.at[rounds - 1])

    def plane_copy(pull_buf, s, q_sem, zt, n):
        at = pull_buf.at[pl.ds(zt * X, n)]
        return pltpu.make_async_remote_copy(
            src_ref=at, dst_ref=at, send_sem=s, recv_sem=q_sem.at[zt],
            device_id=(lax.rem(d + 1, D), r), device_id_type=MESH,
        )

    def gather_a(m, _):
        base = plane(m) * X
        for e in range(X):
            keys(base + e)
        serve(hist_av, send_a, pull_a, a_s, a_r, base, X)
        return 0

    if Z == 4:
        turn = 2 * lax.rem(lax.div(z + 1, 2), 2)
    else:
        turn = 0

    holds = beside if dense and Z == 4 else jnp.logical_and(side == 1, False)

    def gather_b(m, _):
        k = lax.rem(m + turn, Z)
        if Z % 2 == 0:
            k = jnp.where(k < H, H - 1 - k, k)
        base = plane(k) * X
        send_b[pl.ds(base, X)] = pick(hist_bv, base, X)

        @pl.when(jnp.logical_or(k >= H, jnp.logical_not(holds)))
        def _():
            ship(send_b, pull_b, b_s, b_r, base, X)

        return 0

    with scope("gather_a"):
        if Z == 4 and X == 2:
            @pl.when(jnp.logical_not(beside))
            def _():
                for e in range(X):
                    start_block(e)
        else:
            for e in range(X):
                start_block(e)
        lax.fori_loop(1, Z, gather_a, 0)
        pull_a[d] = send_a[d]

    pl.semaphore_wait(stage_sem.at[rounds - 1], len(mates))
    if R == 4:
        signal_rep(stage_sem.at[rounds])
    copies[5].wait()
    held = Z - H * lax.div(turn, H) if Z == 4 else Z
    with scope("gather_b"):
        lax.fori_loop(0, held, gather_b, 0)

    if dense:
        copies[3].wait()
        copies[4].wait()

        def spread_tiles(i, _):
            first = cols[i, home] - far_base
            for p in range(D):
                t = home + lax.rem(p - first + D, D)
                far_v[p // X, pl.ds(i * slots, slots), (p % X) * slots:(p % X + 1) * slots] = vals_v[i, t]
            return 0

        with scope("tiles"):
            lax.fori_loop(0, blocks, spread_tiles, 0)
    if not dense:
        copies[3].wait()
        copies[4].wait()
    late_bytes = sum(math.prod(t.shape) for _, t in loads[prompt:])
    span_all = pl.ds(0, late_bytes // (slots * feat))
    pltpu.make_async_copy(hist_a.at[span_all], hist_av.at[span_all], local_sem.at[prompt]).wait()

    def product(i, picks):
        left = jnp.concatenate([vals_v[i, t] for t, _ in picks], axis=1)
        right = jnp.concatenate([b for _, b in picks], axis=0)
        return jnp.dot(left, right, preferred_element_type=jnp.float32)

    def near_tiles(i, _):
        picks = [(0, cur_v[cols[i, 0]])]
        picks += [(t, hist_av[jnp.maximum(cols[i, t] - blocks, 0)]) for t in range(1, home)]
        acc_a[i] = product(i, picks)
        acc_b[i] = product(i, [(t, hist_bv[jnp.maximum(cols[i, t] - blocks, 0)]) for t in range(1, home)])
        return 0

    with scope("near"):
        lax.fori_loop(0, blocks, near_tiles, 0)
    with scope("gather_b2"):
        lax.fori_loop(held, Z, gather_b, 0)
        pull_b[d] = send_b[d]

    rows = blocks * slots

    def arrive(n, pull_buf, s, q_sem):
        if n == 0 or Z % 2:
            m = (n + Z - 1) % Z
        else:
            m = H + n - 1 if n < H else n - H
        zt = plane(m)
        if n == 0:
            if X > 1:
                plane_copy(pull_buf, s, q_sem, zt, X - 1).wait_recv()
        else:
            plane_copy(pull_buf, s, q_sem, zt, X).wait_recv()

        return zt

    def pull_plane(n, acc_ref, pull_buf, s, q_sem):
        zt = arrive(n, pull_buf, s, q_sem)
        part = jnp.dot(
            far_v[zt], pull_buf[pl.ds(zt * X, X)].reshape(X * slots, feat),
            preferred_element_type=jnp.float32,
        )
        acc_ref[...] += part.reshape(blocks, slots, feat)

    def pull_all(acc_ref, pull_buf, s, q_sem, count=Z):
        if dense:
            for n in range(count):
                pull_plane(n, acc_ref, pull_buf, s, q_sem)
            return

        if X > 1:
            plane_copy(pull_buf, s, q_sem, z, X - 1).wait_recv()

        def one(k, _):
            plane_copy(pull_buf, s, q_sem, lax.rem(z + 1 + k, Z), X).wait_recv()
            return 0

        lax.fori_loop(0, Z - 1, one, 0)

        def far(i, _):
            acc_ref[i] += product(
                i, [(t, pull_buf[jnp.maximum(cols[i, t] - far_base, 0)]) for t in range(home, tiles)]
            )
            return 0

        lax.fori_loop(0, blocks, far, 0)

    factor_two = math.log(strength / 2 + 1.0)
    factor_three = math.log(strength / 3 + 1.0)

    def mix(acc_ref, at):
        return (1.0 - restart) * acc_ref[at] + restart * zero_v[at].astype(jnp.float32)

    def activate(mixed, low, w, factor):
        shape = mixed.shape
        prod = jnp.dot(low.reshape(-1, feat), w[...], preferred_element_type=jnp.float32)
        inner = (1.0 - factor) * mixed + factor * prod.reshape(shape)
        return jnp.maximum(inner, 0.0).astype(jnp.bfloat16)

    with scope("pull_a"):
        pull_all(acc_a, pull_a, a_s, a_r)

    if dense and Z == 4:
        @pl.when(holds)
        def _():
            for m in range(H):
                ship(send_b, pull_b, b_s, b_r, plane(H - 1 - m) * X, X)


    step = 2 if blocks % 2 == 0 else 1
    pieces = blocks // step
    early = pieces

    def fresh_copy(slot, target, k, c, n=1):
        at = pl.ds(c * step, n * step)
        recv = f_r.at[c] if k == 0 else f_r.at[pieces + k - 1]
        return pltpu.make_async_remote_copy(
            src_ref=hist_out.at[slot, at], dst_ref=hist_out.at[slot, at], send_sem=f_s,
            recv_sem=recv, device_id=(d, target), device_id_type=MESH,
        )

    if R == 4:
        mate, across = mates
        targets = [across, mate]
    else:
        mate, across = r + 1 - 2 * side, None
        targets = mates

    def second(c, _):
        at = pl.ds(c * step, step)
        mixed = mix(acc_a, at)
        made = activate(mixed, mixed.astype(jnp.bfloat16), w2_v, factor_two)
        fresh_v[at] = made
        hist_out[r, at] = made
        return 0

    with scope("second"):
        lax.fori_loop(0, pieces, second, 0)

        def send_fresh(c, _):
            for k, t in enumerate(targets):
                fresh_copy(r, t, k, c).start()
            return 0

        lax.fori_loop(0, early, send_fresh, 0)

    def own_tile(i, _):
        acc_b[i] += product(i, [(0, fresh_v[cols[i, 0]])])
        return 0

    with scope("own"):
        lax.fori_loop(0, blocks, own_tile, 0)

    if R == 4:
        pl.semaphore_wait(stage_sem.at[rounds], len(mates))

    with scope("pull_b"):
        pull_all(acc_b, pull_b, b_s, b_r, Z - 1)
        acc_b[...] = mix(acc_b, slice(None))
        last = arrive(Z - 1, pull_b, b_s, b_r) if dense else None
    with scope("grad"):
        mixed = acc_b[...].reshape(rows, feat)
        if dense:
            late = pull_b[pl.ds(last * X, X)].reshape(X * slots, feat)
            part = jnp.dot(far_v[last], late, preferred_element_type=jnp.float32)
            mixed = mixed + (1.0 - restart) * part
            acc_b[...] = mixed.reshape(blocks, slots, feat)
        low = mixed.astype(jnp.bfloat16)
        low_v[...] = low.reshape(blocks, slots, feat)
        grad = factor_three * lax.dot_general(
            low, up_v[...].reshape(rows, feat),
            (((0,), (0,)), ((), ())), preferred_element_type=jnp.float32,
        )
        owners, piece = g_send.shape[:2]
        g_term[...] = grad.reshape(owners, piece, feat)

    pair = r + 1 - 2 * side
    to_mate = pltpu.make_async_remote_copy(
        src_ref=g_term, dst_ref=g_mate, send_sem=g_s, recv_sem=g_r,
        device_id=(d, pair), device_id_type=MESH,
    )

    if R & (R - 1):
        def place(t):
            return lax.div(t, R), lax.rem(t, R)
    else:
        def place(t):
            return lax.shift_right_logical(t, R.bit_length() - 1), jnp.bitwise_and(t, R - 1)

    half = R // 2
    own_part = (d - (H - 1) * X) * half + lax.div(r, 2)
    reduces = jnp.logical_and(side == 1, jnp.logical_and(own_part >= 0, own_part < owners))
    turned = lax.div(owners, 2) * (1 - lax.div(z, H))
    voice = d * half + lax.div(r, 2)

    @pl.when(side == 1)
    def _():
        to_mate.start()

    @pl.when(side == 0)
    def _():
        with scope("mate"):
            to_mate.wait_recv()
        g_send[...] = (g_term[...] + g_mate[...]).astype(g_send.dtype)

        def scatter(k, _):
            o = lax.rem(k + turned, owners)
            pltpu.make_async_remote_copy(
                src_ref=g_send.at[o], dst_ref=g_recv.at[voice], send_sem=g_s, recv_sem=g_r,
                device_id=((H - 1) * X + lax.div(o, half), 2 * lax.rem(o, half) + 1),
                device_id_type=MESH,
            ).start()
            return 0

        for k in range(owners):
            scatter(k, 0)

    lax.fori_loop(early, pieces, send_fresh, 0)

    def third(c, _):
        at = pl.ds(c * step, step)
        layer_out[at] = activate(acc_b[at], low_v[at], w3_v, factor_three)
        return 0

    with scope("third"):
        lax.fori_loop(0, pieces, third, 0)

    def whole(ref, n, s, q):
        part = ref.at[pl.ds(0, n)]
        return pltpu.make_async_remote_copy(
            src_ref=part, dst_ref=part, send_sem=s, recv_sem=q,
            device_id=(lax.rem(d + 1, D), r), device_id_type=MESH,
        )

    @pl.when(reduces)
    def _():
        with scope("scatter"):
            whole(g_recv, N // 2, g_s, g_r).wait_recv()
        g_part[...] = jnp.sum(g_recv[...].astype(jnp.float32), axis=0).astype(g_part.dtype)

        def spread(k, _):
            t = k + jnp.where(k >= me, 1, 0)
            pltpu.make_async_remote_copy(
                src_ref=g_part, dst_ref=g_all.at[own_part], send_sem=p_s, recv_sem=p_r,
                device_id=place(t), device_id_type=MESH,
            ).start()
            return 0

        lax.fori_loop(0, N - 1, spread, 0)
        g_all[own_part] = g_part[...]

    if R == 4:
        def forward(c, _):
            fresh_copy(across, across, 0, c).wait_recv()
            fresh_copy(across, mate, 2, c).start()
            return 0

        with scope("forward"):
            lax.fori_loop(0, pieces, forward, 0)
    with scope("spread"):
        @pl.when(reduces)
        def _():
            whole(g_all, owners - 1, p_s, p_r).wait_recv()

        @pl.when(jnp.logical_not(reduces))
        def _():
            whole(g_all, owners, p_s, p_r).wait_recv()

    grad_res[...] = g_all[...].astype(jnp.float32)

    with scope("drain"):
        if R == 4:
            for k in (1, 2):
                fresh_copy(r, mate, k, 0, pieces).wait_recv()
        else:
            def landed(c, _):
                fresh_copy(r, mate, 0, c).wait_recv()
                return 0

            lax.fori_loop(0, pieces, landed, 0)
            for k in range(1, R - 1):
                fresh_copy(r, mate, k, 0, pieces).wait_recv()
        whole(hist_out, R - 1, f_s, p_r).wait_send()
        whole(ask, D - 1, idx_s, p_r).wait_send()
        whole(send_a, D - 1, a_s, p_r).wait_send()
        whole(send_b, D - 1, b_s, p_r).wait_send()

        @pl.when(reduces)
        def _():
            def sent(k, _):
                pltpu.make_async_remote_copy(
                    src_ref=g_part, dst_ref=g_all.at[own_part], send_sem=p_s, recv_sem=p_r,
                    device_id=(d, pair), device_id_type=MESH,
                ).wait_send()
                return 0

            lax.fori_loop(0, N - 1, sent, 0)

        @pl.when(side == 1)
        def _():
            to_mate.wait_send()

        @pl.when(side == 0)
        def _():
            whole(g_send, owners, g_s, g_r).wait_send()


def hand_over(parts, *refs):
    sources, targets, sem = refs[:3], refs[3:6], refs[6]
    outs = []
    order = (1, 0, 2)
    for n, src, dst in [(parts[k], sources[k], targets[k]) for k in order]:
        rows = src.shape[0] // n
        for i in range(n):
            at = pl.ds(i * rows, rows)
            outs.append(pltpu.make_async_copy(src.at[at], dst.at[at], sem.at[len(outs)]))
    for c in outs:
        c.start()
    for c in outs:
        c.wait()


def local(D, R, h_zero, h_prev, hist_a, hist_b, tile_vals, tile_cols, pull_rows, pull_counts,
          weight_two, weight_three, grad_out):
    blocks, tiles, tile = tile_vals.shape[:3]
    feat = hist_a.shape[1]
    N = D * R
    hist_blocks = hist_a.shape[0] // tile
    bf, f32 = jnp.bfloat16, jnp.float32
    own = (blocks, tile, feat)
    hist = (hist_blocks, tile, feat)
    slots = pull_rows.shape[2]
    pulled = (D, slots, feat)
    X = 2 if D % 2 == 0 else 1
    Z = D // X
    dense = tiles - 4 == D
    owners = X * R
    piece = feat // owners
    far = (Z, blocks * tile, X * tile) if dense else (1, 16, 128)
    pieces = blocks // 2 if blocks % 2 == 0 else blocks
    links = max(R - 1, 3)
    vm = pltpu.VMEM
    dma = pltpu.SemaphoreType.DMA
    any_spec = pl.BlockSpec(memory_space=pl.ANY)
    vspec = pl.BlockSpec(memory_space=pltpu.VMEM)
    grant = 24 * 2**20 + D * slots * (8 * feat + 8 * slots)
    out3, fresh, grad = pl.pallas_call(
        functools.partial(kernel, D, R),
        out_shape=(
            jax.ShapeDtypeStruct(own, bf),
            jax.ShapeDtypeStruct((R,) + own, bf),
            jax.ShapeDtypeStruct((owners, piece, feat), f32),
        ),
        in_specs=[any_spec] * 11,
        out_specs=(vspec, vspec, vspec),
        scratch_shapes=[
            pltpu.SMEM(tile_cols.shape, jnp.int32), pltpu.SMEM(pull_counts.shape, jnp.int32),
            vm(pull_rows.shape, jnp.int32),
            vm(own, bf), vm(own, bf), vm(hist, bf), vm(hist, bf), vm(tile_vals.shape, bf), vm(far, bf),
            vm((feat, feat), bf), vm((feat, feat), bf), vm(own, bf),
            vm((D, 1, slots), jnp.int32), vm((D, 1, slots), jnp.int32),
            vm((D, slots, slots), bf), vm((D, slots, X * slots), bf),
            vm(pulled, bf), vm(pulled, bf), vm(pulled, bf), vm(pulled, bf),
            vm(own, f32), vm(own, f32),
            vm(own, bf), vm(own, bf),
            vm((owners, piece, feat), f32), vm((owners, piece, feat), f32),
            vm((owners, piece, feat), bf), vm((N // 2, piece, feat), bf),
            vm((piece, feat), bf), vm((owners, piece, feat), bf),
            dma((7,)), pltpu.SemaphoreType.REGULAR((Z + X - 1,)),
            dma, dma((D,)), dma, dma((Z,)), dma, dma((Z,)),
            dma, dma((pieces + links - 1,)), dma, dma, dma, dma,
        ],
        compiler_params=pltpu.CompilerParams(
            collective_id=0, has_side_effects=True, vmem_limit_bytes=grant
        ),
    )(
        *[
            pltpu.with_memory_space_constraint(x, pltpu.HBM)
            for x in (
                tile_cols, pull_counts, pull_rows, h_zero.reshape(own), h_prev.reshape(own),
                hist_a.reshape(hist), hist_b.reshape(hist), tile_vals, weight_two, weight_three,
                grad_out.reshape(own),
            )
        ]
    )
    flat = (
        out3.reshape(h_zero.shape),
        fresh.reshape(R * h_zero.shape[0], feat),
        grad.reshape(feat, feat),
    )
    parts = (1, 1, 1)
    return pl.pallas_call(
        functools.partial(hand_over, parts),
        out_shape=tuple(jax.ShapeDtypeStruct(x.shape, x.dtype) for x in flat),
        in_specs=[vspec] * 3,
        out_specs=(any_spec,) * 3,
        scratch_shapes=[dma((sum(parts),))],
        compiler_params=pltpu.CompilerParams(vmem_limit_bytes=8 * 1024 * 1024),
    )(*flat)


def solution(mesh):
    both = ("dev", "rep")
    return jax.shard_map(
        functools.partial(local, mesh.shape["dev"], mesh.shape["rep"]),
        mesh=mesh,
        in_specs=(
            P(both, None), P(both, None), P("dev", None), P("dev", None),
            P(both, None, None, None), P(both, None), P(both, None, None), P(both, None),
            P(), P(), P(both, None),
        ),
        out_specs=(P(both, None), P("dev", None), P()),
        check_vma=False,
    )
```
